8 devices in a mesh: data: 2 (over z, y), expert: 4 (over x, core).
Axes of the slice: x: 2, y: 2, z: 1, core: 2. Of those that a mesh axis runs over, the one named last changes fastest.
Arguments:
- tok_x: bfloat16 [12288, 768], P(('data', 'expert')), parts along dimension 0
- route_idx: int32 [12288, 1], P(('data', 'expert')), parts along dimension 0
- route_gate: float32 [12288, 1], P(('data', 'expert')), parts along dimension 0
- grad_y: bfloat16 [12288, 768], P(('data', 'expert')), parts along dimension 0
- w_gate: bfloat16 [256, 768, 256], P('expert')
- w_up: bfloat16 [256, 768, 256], P('expert')
- w_down: bfloat16 [256, 256, 768], P('expert')
Outputs:
- output 1: bfloat16 [12288, 768], P(('data', 'expert')), parts along dimension 0
- output 2: bfloat16 [12288, 768], P(('data', 'expert')), parts along dimension 0
- output 3: float32 [512, 768, 256], P(('data', 'expert')), parts along dimension 0
- output 4: float32 [512, 768, 256], P(('data', 'expert')), parts along dimension 0
- output 5: float32 [512, 256, 768], P(('data', 'expert')), parts along dimension 0
There are 2 independent parts. The reference program is written for one: setup_inputs(seed, part) draws one part's arguments, and reference() takes and returns one part's arrays. A program takes and returns all parts, laid end to end along the dimension named above; an argument that names none is the same for every part.
All inputs are finite; a program needn't handle non-finite values.
Results may differ from the reference program's by a relative error of at most 0.0094902.
Values are sent between devices in bfloat16 or wider.
A program may use at most 1 GiB of HBM per device.

```python
import jax
import jax.numpy as jnp
from jax import lax

GROUP_SIZE = 4
TOKENS = 1536
MODEL_DIM = 768
FFN_DIM = 256
EXPERTS = 256
TOP_K = 1

HOT_COUNT = min(4, EXPERTS // 8)
HOT_STRIDE = EXPERTS // HOT_COUNT
COLD_COUNT = EXPERTS - HOT_COUNT
CAPACITY = max(4, 2 * TOKENS * TOP_K // EXPERTS)
FILL_ROWS = CAPACITY + 4
PART_ROWS = GROUP_SIZE * TOKENS
SLOT_COUNT = TOKENS * TOP_K


def draw_routing(route_key):
    key_list = jax.random.split(route_key, 5)
    row_ids = jnp.arange(PART_ROWS)
    slot_ids = jnp.arange(TOP_K)
    cold_first = jax.random.randint(key_list[0], (PART_ROWS,), 0, COLD_COUNT)
    cold_second = jax.random.randint(key_list[1], (PART_ROWS,), 0, 2 * COLD_COUNT)
    forced = jax.random.randint(key_list[2], (GROUP_SIZE,), 0, COLD_COUNT)
    is_fill = (row_ids % TOKENS) < FILL_ROWS
    cold_base = jnp.where(is_fill, (forced[row_ids // TOKENS] - (TOP_K - 1)) % COLD_COUNT, jnp.minimum(cold_first, cold_second))
    cold_rank = (cold_base[:, None] + slot_ids[None, :]) % COLD_COUNT
    cold_ids = (cold_rank // (HOT_STRIDE - 1)) * HOT_STRIDE + 1 + cold_rank % (HOT_STRIDE - 1)
    hot_roll = jax.random.randint(key_list[3], (PART_ROWS, TOP_K), 0, 10)
    hot_base = jax.random.randint(key_list[4], (PART_ROWS,), 0, HOT_COUNT)
    hot_ids = ((hot_base[:, None] + slot_ids[None, :]) % HOT_COUNT) * HOT_STRIDE
    use_hot = (hot_roll < 6) & (slot_ids[None, :] < min(HOT_COUNT, TOP_K)) & jnp.logical_not(is_fill)[:, None]
    return jnp.where(use_hot, hot_ids, cold_ids).astype(jnp.int32)


def setup_inputs(seed: int = 0, part: int = 0) -> dict:
    root_key = jax.random.key(seed)
    part_key = jax.random.fold_in(root_key, part)
    tok_keys = jax.random.split(part_key, 4)
    weight_keys = jax.random.split(root_key, 3)
    tok_x = jax.random.normal(tok_keys[0], (PART_ROWS, MODEL_DIM), jnp.float32).astype(jnp.bfloat16)
    route_idx = draw_routing(tok_keys[1])
    route_gate = jax.random.uniform(tok_keys[2], (PART_ROWS, TOP_K), jnp.float32, 0.2, 1.0)
    grad_y = jax.random.normal(tok_keys[3], (PART_ROWS, MODEL_DIM), jnp.float32).astype(jnp.bfloat16)
    in_scale = MODEL_DIM ** -0.5
    w_gate = (jax.random.normal(weight_keys[0], (EXPERTS, MODEL_DIM, FFN_DIM), jnp.float32) * in_scale).astype(jnp.bfloat16)
    w_up = (jax.random.normal(weight_keys[1], (EXPERTS, MODEL_DIM, FFN_DIM), jnp.float32) * in_scale).astype(jnp.bfloat16)
    w_down = (jax.random.normal(weight_keys[2], (EXPERTS, FFN_DIM, MODEL_DIM), jnp.float32) * FFN_DIM ** -0.5).astype(jnp.bfloat16)
    return {'tok_x': tok_x, 'route_idx': route_idx, 'route_gate': route_gate, 'grad_y': grad_y, 'w_gate': w_gate, 'w_up': w_up, 'w_down': w_down}


def silu_parts(pre_act):
    sigmoid_a = jax.nn.sigmoid(pre_act)
    return pre_act * sigmoid_a, sigmoid_a * (1.0 + pre_act * (1.0 - sigmoid_a))


def expert_rows(rows_x, row_gate, rows_dy, w_in, w_lin, w_out):
    pre_a = jnp.dot(rows_x, w_in, preferred_element_type=jnp.float32).astype(jnp.bfloat16)
    pre_b = jnp.dot(rows_x, w_lin, preferred_element_type=jnp.float32).astype(jnp.bfloat16)
    silu_a, silu_slope = silu_parts(pre_a.astype(jnp.float32))
    lin_b = pre_b.astype(jnp.float32)
    hidden = (silu_a * lin_b).astype(jnp.bfloat16)
    out_rows = jnp.dot(hidden, w_out, preferred_element_type=jnp.float32).astype(jnp.bfloat16)
    grad_out = (row_gate[:, None] * rows_dy.astype(jnp.float32)).astype(jnp.bfloat16)
    grad_h = jnp.dot(grad_out, w_out.T, preferred_element_type=jnp.float32).astype(jnp.bfloat16).astype(jnp.float32)
    grad_a = (grad_h * lin_b * silu_slope).astype(jnp.bfloat16)
    grad_b = (grad_h * silu_a).astype(jnp.bfloat16)
    grad_in = (jnp.dot(grad_a, w_in.T, preferred_element_type=jnp.float32) + jnp.dot(grad_b, w_lin.T, preferred_element_type=jnp.float32)).astype(jnp.bfloat16)
    grad_w_in = jnp.dot(rows_x.T, grad_a, preferred_element_type=jnp.float32)
    grad_w_lin = jnp.dot(rows_x.T, grad_b, preferred_element_type=jnp.float32)
    grad_w_out = jnp.dot(hidden.T, grad_out, preferred_element_type=jnp.float32)
    return out_rows, grad_in, grad_w_in, grad_w_lin, grad_w_out


def route_device(dev_idx):
    flat_ids = dev_idx.reshape(SLOT_COUNT)
    onehot = (flat_ids[:, None] == jnp.arange(EXPERTS, dtype=jnp.int32)[None, :]).astype(jnp.int32)
    position = jnp.sum(jnp.cumsum(onehot, axis=0) * onehot, axis=1) - 1
    is_kept = (flat_ids % HOT_STRIDE != 0) & (position < CAPACITY)
    dest_row = jnp.where(is_kept, flat_ids * CAPACITY + position, EXPERTS * CAPACITY)
    slot_src = jnp.full((EXPERTS * CAPACITY + 1,), SLOT_COUNT, jnp.int32).at[dest_row].set(jnp.arange(SLOT_COUNT, dtype=jnp.int32))
    return dest_row, slot_src[:EXPERTS * CAPACITY]


def take_rows(row_table, row_ids):
    return row_table[row_ids]


def reference(tok_x, route_idx, route_gate, grad_y, w_gate, w_up, w_down):
    dest_row, slot_src = jax.vmap(route_device)(route_idx.reshape(GROUP_SIZE, TOKENS, TOP_K))
    tok_src = slot_src // TOP_K
    zero_rows = jnp.zeros((GROUP_SIZE, 1, MODEL_DIM), jnp.bfloat16)
    x_pad = jnp.concatenate([tok_x.reshape(GROUP_SIZE, TOKENS, MODEL_DIM), zero_rows], axis=1)
    dy_pad = jnp.concatenate([grad_y.reshape(GROUP_SIZE, TOKENS, MODEL_DIM), zero_rows], axis=1)
    gate_pad = jnp.concatenate([route_gate.reshape(GROUP_SIZE, SLOT_COUNT), jnp.zeros((GROUP_SIZE, 1), jnp.float32)], axis=1)
    buf_x = jax.vmap(take_rows)(x_pad, tok_src).reshape(GROUP_SIZE, EXPERTS, CAPACITY, MODEL_DIM)
    buf_dy = jax.vmap(take_rows)(dy_pad, tok_src).reshape(GROUP_SIZE, EXPERTS, CAPACITY, MODEL_DIM)
    buf_gate = jax.vmap(take_rows)(gate_pad, slot_src).reshape(GROUP_SIZE, EXPERTS, CAPACITY)
    ex_x = jnp.swapaxes(buf_x, 0, 1).reshape(EXPERTS, GROUP_SIZE * CAPACITY, MODEL_DIM)
    ex_dy = jnp.swapaxes(buf_dy, 0, 1).reshape(EXPERTS, GROUP_SIZE * CAPACITY, MODEL_DIM)
    ex_gate = jnp.swapaxes(buf_gate, 0, 1).reshape(EXPERTS, GROUP_SIZE * CAPACITY)
    cold_out, cold_dx, cold_dwg, cold_dwu, cold_dwd = lax.map(lambda operands: expert_rows(*operands), (ex_x, ex_gate, ex_dy, w_gate, w_up, w_down))
    back_out = jnp.swapaxes(cold_out.reshape(EXPERTS, GROUP_SIZE, CAPACITY, MODEL_DIM), 0, 1).reshape(GROUP_SIZE, EXPERTS * CAPACITY, MODEL_DIM)
    back_dx = jnp.swapaxes(cold_dx.reshape(EXPERTS, GROUP_SIZE, CAPACITY, MODEL_DIM), 0, 1).reshape(GROUP_SIZE, EXPERTS * CAPACITY, MODEL_DIM)
    out_slots = jax.vmap(take_rows)(jnp.concatenate([back_out, zero_rows], axis=1), dest_row).reshape(PART_ROWS, TOP_K, MODEL_DIM)
    dx_slots = jax.vmap(take_rows)(jnp.concatenate([back_dx, zero_rows], axis=1), dest_row).reshape(PART_ROWS, TOP_K, MODEL_DIM)
    hot_ids = jnp.arange(HOT_COUNT, dtype=jnp.int32) * HOT_STRIDE
    hot_gate = jnp.sum(jnp.where(route_idx[:, :, None] == hot_ids[None, None, :], route_gate[:, :, None], 0.0), axis=1)
    hot_out, hot_dx, hot_dwg, hot_dwu, hot_dwd = lax.map(lambda operands: expert_rows(tok_x, operands[0], grad_y, operands[1], operands[2], operands[3]), (hot_gate.T, w_gate[::HOT_STRIDE], w_up[::HOT_STRIDE], w_down[::HOT_STRIDE]))
    out_y = jnp.sum(route_gate[:, :, None] * out_slots.astype(jnp.float32), axis=1) + jnp.sum(hot_gate.T[:, :, None] * hot_out.astype(jnp.float32), axis=0)
    grad_x = jnp.sum(dx_slots.astype(jnp.float32), axis=1) + jnp.sum(hot_dx.astype(jnp.float32), axis=0)
    grad_w_gate = cold_dwg.at[::HOT_STRIDE].add(hot_dwg)
    grad_w_up = cold_dwu.at[::HOT_STRIDE].add(hot_dwu)
    grad_w_down = cold_dwd.at[::HOT_STRIDE].add(hot_dwd)
    return (out_y.astype(jnp.bfloat16), grad_x.astype(jnp.bfloat16), grad_w_gate, grad_w_up, grad_w_down)
```

```python
import functools

import jax
import jax.numpy as jnp
from jax import lax
from jax.experimental import pallas as pl
from jax.experimental.pallas import tpu as pltpu
from jax.sharding import PartitionSpec as P

BF16, F32, I32 = jnp.bfloat16, jnp.float32, jnp.int32
WIN = 32
LIST = 4096
COL_ROUNDS, COL_HI, COL_LO = 66, 128, 192


def iota(shape, dim):
    return lax.broadcasted_iota(I32, shape, dim)


def exact_dot(lhs, rhs):
    return jnp.dot(lhs, rhs, precision=lax.Precision.HIGHEST, preferred_element_type=F32)


def mm(lhs, rhs):
    return jnp.dot(lhs, rhs, preferred_element_type=F32)


def mm_nt(lhs, rhs):
    return lax.dot_general(lhs, rhs, (((1,), (1,)), ((), ())), preferred_element_type=F32)


def mm_tn(lhs, rhs):
    return lax.dot_general(lhs, rhs, (((0,), (0,)), ((), ())), preferred_element_type=F32)


def to_column(row):
    wide = jnp.broadcast_to(row, (128, row.shape[1]))
    return jnp.transpose(wide)[:, :1]


def route_kernel(capacity, caps, ids_ref, vslot_ref, tbl_ref, pos_ref):
    blocks = ids_ref.shape[1] // 256
    er = iota((256, 256), 0)
    ec = iota((256, 256), 1)
    upper = jnp.where(er < ec, 1.0, 0.0).astype(BF16)
    carry = jnp.zeros((256, 1), F32)
    for b in range(blocks):
        span = slice(b * 256, (b + 1) * 256)
        oh = jnp.where(er == ids_ref[:, span], 1.0, 0.0)
        cum = mm(oh.astype(BF16), upper) + carry
        pos_ref[:, span] = jnp.sum(oh * cum, axis=0, keepdims=True)
        carry = carry + jnp.sum(oh, axis=1, keepdims=True)
    hot = (er[:, :1] & 63) == 0
    cnt = jnp.where(hot, carry, jnp.minimum(carry, float(capacity)))
    cold_cnt = jnp.broadcast_to(jnp.where(hot, 0.0, cnt), (256, 128))
    dr, dc = er >> 6, ec >> 6
    same = jnp.where(dr == dc, 1.0, 0.0)
    cold_tot = exact_dot(same, cold_cnt)[:, :1]
    rel = exact_dot(jnp.where(ec < er, same, 0.0), cold_cnt)[:, :1]
    rounds = jnp.ones((256, 1), F32)
    for k in range(1, 1 + ids_ref.shape[1] // min(caps)):
        more = (cold_tot > float(k * caps[0])) | (hot & (cnt > float(k * caps[1])))
        rounds = rounds + jnp.where(more, 1.0, 0.0)
    rounds = jnp.max(rounds, axis=0, keepdims=True)
    lm = er & 63
    rel_hi = jnp.floor(rel * 0.0625)
    table = jnp.where((ec == lm) & (lm > 0), cnt, 0.0)
    table += jnp.where(ec == lm + COL_HI, rel_hi, 0.0) + jnp.where(ec == lm + COL_LO, rel - 16.0 * rel_hi, 0.0)
    table += jnp.where((ec == COL_ROUNDS) & (lm == 0), rounds, 0.0)
    pick = jnp.where((iota((8, 256), 1) >> 6) == iota((8, 256), 0), 1.0, 0.0)
    tbl_ref[...] = exact_dot(pick, table)
    start = (dr[:, :1] * LIST).astype(F32) + jnp.where(hot, float(4 * LIST), rel)
    for b in range(blocks):
        span = slice(b * 256, (b + 1) * 256)
        ids = ids_ref[:, span]
        pos = pos_ref[:, span]
        mine = jnp.sum(jnp.where(er == ids, start, 0.0), axis=0, keepdims=True)
        kept = ((ids & 63) == 0) | (pos < float(capacity))
        vslot_ref[:, span] = jnp.where(kept, mine + pos, -1.0).astype(I32)


def pack_kernel(first_list, cap, round_ref, vslot_ref, gate_ref, x_ref, dy_ref, tbl_ref, send_ref, g_ref):
    step = pl.program_id(0)
    tok_n, d = x_ref.shape
    rows_n = send_ref.shape[0]

    @pl.when(step == 0)
    def _():
        for b in range(tok_n // 256):
            span = slice(b * 256, (b + 1) * 256)
            gate = to_column(gate_ref[:, span])
            g_ref[span, :] = (gate * dy_ref[span, :].astype(F32)).astype(BF16)

    row = iota((rows_n, tok_n), 0)
    want = row + (first_list + step) * LIST + round_ref[0] * cap
    if cap < rows_n:
        want = jnp.where(row < cap, want, -2)
    perm = jnp.where(want == vslot_ref[...], 1.0, 0.0).astype(BF16)
    x = mm(perm, x_ref[...])
    if cap < rows_n:
        tbl = tbl_ref[pl.ds(step, 1), :]
        tbl = jnp.concatenate([tbl, jnp.zeros((1, d - tbl.shape[1]), F32)], axis=1)
        x = jnp.where(iota(x.shape, 0) == cap, tbl, x)
    send_ref[:, :d] = x.astype(BF16)
    send_ref[:, d:] = mm(perm, g_ref[...]).astype(BF16)


def forward(rows_x, w1, w3, w2):
    a = mm(rows_x, w1).astype(BF16).astype(F32)
    b = mm(rows_x, w3).astype(BF16).astype(F32)
    s = jax.nn.sigmoid(a)
    silu = a * s
    h = (silu * b).astype(BF16)
    out = mm(h, w2).astype(BF16)
    return a, b, s, silu, h, out


def backward(fwd, rows_g, w1, w3, w2):
    a, b, s, silu, h, out = fwd
    dh = mm_nt(rows_g, w2).astype(BF16).astype(F32)
    da = (dh * b * (s * (1.0 + a * (1.0 - s)))).astype(BF16)
    db = (dh * silu).astype(BF16)
    dx = (mm_nt(da, w1) + mm_nt(db, w3)).astype(BF16)
    return da, db, dx


def window(tbl_ref, src, expert, slab, rows_n):
    first = src * slab + tbl_ref[src, 64 + expert]
    count = tbl_ref[src, expert]
    base = pl.multiple_of(jnp.minimum((first // 16) * 16, rows_n - WIN), 16)
    return base, first - base, count


def inside(shape, off, count):
    r = iota(shape, 0)
    return (r >= off) & (r < off + count)


def load_rows(xg_ref, tbl_ref, expert, srcs, slab):
    parts = []
    for src in range(srcs):
        base, off, count = window(tbl_ref, src, expert, slab, xg_ref.shape[0])
        rows = xg_ref[pl.ds(base, WIN), :]
        parts.append(jnp.where(inside(rows.shape, off, count), rows, jnp.zeros_like(rows)))
    return jnp.concatenate(parts, axis=0)


def cold_kernel(srcs, slab, tbl_ref, xg_ref, w1_ref, w3_ref, w2_ref, od_ref, hab_ref):
    step = pl.program_id(0)
    expert = step + 1
    d = w1_ref.shape[1]

    @pl.when(step == 0)
    def _():
        od_ref[...] = jnp.zeros_like(od_ref)
        hab_ref[...] = jnp.zeros_like(hab_ref)

    rows = load_rows(xg_ref, tbl_ref, expert, srcs, slab)
    w1, w3, w2 = w1_ref[0], w3_ref[0], w2_ref[0]
    fwd = forward(rows[:, :d], w1, w3, w2)
    da, db, dx = backward(fwd, rows[:, d:], w1, w3, w2)
    od = jnp.concatenate([fwd[5], dx], axis=1)
    hab = jnp.concatenate([fwd[4], da, db], axis=1)
    for src in range(srcs):
        base, off, count = window(tbl_ref, src, expert, slab, xg_ref.shape[0])
        at = pl.ds(base, WIN)
        span = slice(src * WIN, (src + 1) * WIN)
        for ref, new in ((od_ref, od[span]), (hab_ref, hab[span])):
            ref[at, :] = jnp.where(inside(new.shape, off, count), new, ref[at, :])


def hot_kernel(xg_ref, w1_ref, w3_ref, w2_ref, od_ref, g1_ref, g3_ref, g2_ref):
    step = pl.program_id(0)
    d = w1_ref.shape[1]
    x, g = xg_ref[:, :d], xg_ref[:, d:]
    w1, w3, w2 = w1_ref[0], w3_ref[0], w2_ref[0]
    fwd = forward(x, w1, w3, w2)
    da, db, dx = backward(fwd, g, w1, w3, w2)
    od_ref[:, :d] = fwd[5]
    od_ref[:, d:] = dx

    @pl.when(step == 0)
    def _():
        for ref in (g1_ref, g3_ref, g2_ref):
            ref[...] = jnp.zeros_like(ref)

    g1_ref[...] += mm_tn(x, da)
    g3_ref[...] += mm_tn(x, db)
    g2_ref[...] += mm_tn(fwd[4], g)


def grad_kernel(srcs, slab, tbl_ref, xg_ref, hab_ref, h1_ref, h3_ref, h2_ref, g1_ref, g3_ref, g2_ref):
    expert = pl.program_id(0)
    d, f = h1_ref.shape

    @pl.when(expert == 0)
    def _():
        g1_ref[0] = h1_ref[...]
        g3_ref[0] = h3_ref[...]
        g2_ref[0] = h2_ref[...]

    @pl.when(expert > 0)
    def _():
        rows = load_rows(xg_ref, tbl_ref, expert, srcs, slab)
        hab = jnp.concatenate([hab_ref[pl.ds(window(tbl_ref, s, expert, slab, xg_ref.shape[0])[0], WIN), :] for s in range(srcs)], axis=0)
        x, g = rows[:, :d], rows[:, d:]
        g1_ref[0] = mm_tn(x, hab[:, f:2 * f])
        g3_ref[0] = mm_tn(x, hab[:, 2 * f:])
        g2_ref[0] = mm_tn(hab[:, :f], g)


def combine_kernel(first_list, cap, slab, round_ref, vslot_ref, gate_ref, ret_ref, *refs):
    y_ref, dx_ref = refs[-2:]
    d = y_ref.shape[1]
    vslot = to_column(vslot_ref[...].astype(F32))
    lane = iota((1, ret_ref.shape[0]), 1)
    dest = jnp.zeros_like(lane)
    for k in range(1, ret_ref.shape[0] // slab):
        dest += jnp.where(lane >= k * slab, 1, 0)
    row = lane - dest * slab
    have = jnp.where(row < cap, (dest + first_list) * LIST + round_ref[0] * cap + row, -2).astype(F32)
    pick = jnp.where(have == vslot, 1.0, 0.0).astype(BF16)
    y = (to_column(gate_ref[...]) * mm(pick, ret_ref[:, :d])).astype(BF16)
    dx = mm(pick, ret_ref[:, d:]).astype(BF16)
    if len(refs) == 4:
        y = y + refs[0][...]
        dx = dx + refs[1][...]
    y_ref[...] = y
    dx_ref[...] = dx


def params(mib):
    return pltpu.CompilerParams(vmem_limit_bytes=mib * 2 ** 20, dimension_semantics=('arbitrary',))


def cost(flops, nbytes):
    return pl.CostEstimate(flops=int(flops), bytes_accessed=int(nbytes), transcendentals=0)


def prefetched(grid, in_specs, out_specs, scratch=()):
    return pltpu.PrefetchScalarGridSpec(num_scalar_prefetch=1, grid=grid, in_specs=in_specs, out_specs=out_specs, scratch_shapes=list(scratch))


COLD_SLAB, COLD_CAP, HOT_SLAB = 272, 271, 288


def solution(mesh):
    srcs = mesh.shape['expert']
    tok_spec = P(('data', 'expert'))
    weight_spec = P('expert')
    whole = functools.partial(pl.BlockSpec, pipeline_mode=pl.Buffered(1))
    sds = jax.ShapeDtypeStruct
    fixed = lambda i, t: (0, 0)

    def shard_body(tok_x, route_idx, route_gate, grad_y, w_gate, w_up, w_down):
        tok_n, d = tok_x.shape
        local_n, _, f = w_gate.shape
        capacity = max(4, 2 * tok_n // (local_n * srcs))
        ids_row = route_idx.reshape(1, tok_n)
        gate_row = route_gate.reshape(1, tok_n)
        w_bytes = local_n * 3 * d * f * 2
        cold_rows, hot_rows = srcs * COLD_SLAB, srcs * HOT_SLAB

        vslot, tbl = pl.pallas_call(
            functools.partial(route_kernel, capacity, (COLD_CAP, HOT_SLAB)),
            out_shape=[sds((1, tok_n), I32), sds((8, 256), F32)],
            scratch_shapes=[pltpu.VMEM((1, tok_n), F32)],
            name='route',
        )(ids_row)

        def pack(rnd, first_list, cap, slab):
            return pl.pallas_call(
                functools.partial(pack_kernel, first_list, cap),
                grid_spec=prefetched(
                    (srcs,),
                    [whole((1, tok_n), fixed), whole((1, tok_n), fixed), whole((tok_n, d), fixed), whole((tok_n, d), fixed), whole((8, 256), fixed)],
                    pl.BlockSpec((slab, 2 * d), lambda i, t: (i, 0)),
                    [pltpu.VMEM((tok_n, d), BF16)],
                ),
                out_shape=sds((srcs * slab, 2 * d), BF16),
                compiler_params=params(48),
                cost_estimate=cost(2 * srcs * slab * tok_n * 2 * d, 2 * tok_n * d * 4),
                name='pack',
            )(rnd, vslot, gate_row, tok_x, grad_y, tbl)

        def exchange(rows, slab):
            return lax.all_to_all(rows.reshape(srcs, slab, 2 * d), 'expert', 0, 0).reshape(srcs * slab, 2 * d)

        def combine(rnd, first_list, cap, slab, ret, parts):
            blk = pl.BlockSpec((256, d), lambda i, t: (i, 0))
            row = pl.BlockSpec((1, 256), lambda i, t: (0, i))
            return pl.pallas_call(
                functools.partial(combine_kernel, first_list, cap, slab),
                grid_spec=prefetched((tok_n // 256,), [row, row, whole((srcs * slab, 2 * d), fixed)] + [blk] * len(parts), [blk, blk]),
                out_shape=[sds((tok_n, d), BF16), sds((tok_n, d), BF16)],
                compiler_params=params(48),
                cost_estimate=cost(2 * tok_n * srcs * slab * 2 * d, srcs * slab * 2 * d * 4),
                name='combine',
            )(rnd, vslot, gate_row, ret, *parts)

        def one_round(rnd):
            cold_xg = exchange(pack(rnd, 0, COLD_CAP, COLD_SLAB), COLD_SLAB)
            hot_xg = exchange(pack(rnd, srcs, HOT_SLAB, HOT_SLAB), HOT_SLAB)
            heads = cold_xg.reshape(srcs, COLD_SLAB, 2 * d)[:, COLD_CAP, :256].astype(I32)
            rel = heads[:, COL_HI:COL_HI + local_n] * 16 + heads[:, COL_LO:COL_LO + local_n] - rnd[0] * COLD_CAP
            end = jnp.clip(rel + heads[:, :local_n], 0, COLD_CAP)
            rel = jnp.clip(rel, 0, COLD_CAP)
            win_tbl = jnp.concatenate([end - rel, rel], axis=1)
            rounds = jnp.max(heads[:, COL_ROUNDS])

            cold_od, cold_hab = pl.pallas_call(
                functools.partial(cold_kernel, srcs, COLD_SLAB),
                grid_spec=prefetched(
                    (local_n - 1,),
                    [whole((cold_rows, 2 * d), fixed), pl.BlockSpec((1, d, f), lambda i, t: (i + 1, 0, 0)), pl.BlockSpec((1, d, f), lambda i, t: (i + 1, 0, 0)), pl.BlockSpec((1, f, d), lambda i, t: (i + 1, 0, 0))],
                    [whole((cold_rows, 2 * d), fixed), whole((cold_rows, 3 * f), fixed)],
                ),
                out_shape=[sds((cold_rows, 2 * d), BF16), sds((cold_rows, 3 * f), BF16)],
                compiler_params=params(48),
                cost_estimate=cost(2 * 6 * 512 * local_n * d * f, w_bytes),
                name='cold',
            )(win_tbl, cold_xg, w_gate, w_up, w_down)
            cold_ret = exchange(cold_od, COLD_SLAB)

            first = lambda i: (0, 0, 0)
            flat = lambda i: (0, 0)
            hot_blk = pl.BlockSpec((hot_rows // 2, 2 * d), lambda i: (i, 0))
            hot_od, hot1, hot3, hot2 = pl.pallas_call(
                hot_kernel,
                grid=(2,),
                in_specs=[hot_blk, whole((1, d, f), first), whole((1, d, f), first), whole((1, f, d), first)],
                out_specs=[hot_blk, whole((d, f), flat), whole((d, f), flat), whole((f, d), flat)],
                out_shape=[sds((hot_rows, 2 * d), BF16), sds((d, f), F32), sds((d, f), F32), sds((f, d), F32)],
                compiler_params=params(48),
                cost_estimate=cost(2 * 9 * hot_rows * d * f, 4 * hot_rows * d * 4),
                name='hot',
            )(hot_xg, w_gate, w_up, w_down)
            hot_ret = exchange(hot_od, HOT_SLAB)

            out3 = lambda i, t: (i, 0, 0)
            grads = pl.pallas_call(
                functools.partial(grad_kernel, srcs, COLD_SLAB),
                grid_spec=prefetched(
                    (local_n,),
                    [whole((cold_rows, 2 * d), fixed), whole((cold_rows, 3 * f), fixed), whole((d, f), fixed), whole((d, f), fixed), whole((f, d), fixed)],
                    [pl.BlockSpec((1, d, f), out3), pl.BlockSpec((1, d, f), out3), pl.BlockSpec((1, f, d), out3)],
                ),
                out_shape=[sds((local_n, d, f), F32), sds((local_n, d, f), F32), sds((local_n, f, d), F32)],
                compiler_params=params(48),
                cost_estimate=cost(2 * 3 * 512 * local_n * d * f, 2 * w_bytes),
                name='grads',
            )(win_tbl, cold_xg, cold_hab, hot1, hot3, hot2)

            parts = combine(rnd, 0, COLD_CAP, COLD_SLAB, cold_ret, ())
            y, dx = combine(rnd, srcs, HOT_SLAB, HOT_SLAB, hot_ret, parts)
            return rounds, (y, dx, *grads)

        rounds, outs = one_round(jnp.zeros((1,), I32))

        def more(state):
            return state[0][0] < rounds

        def again(state):
            _, extra = one_round(state[0])
            return (state[0] + 1, *(a + b for a, b in zip(state[1:], extra)))

        return lax.while_loop(more, again, (jnp.ones((1,), I32), *outs))[1:]

    return jax.shard_map(shard_body, mesh=mesh, in_specs=(tok_spec, tok_spec, tok_spec, tok_spec, weight_spec, weight_spec, weight_spec), out_specs=(tok_spec,) * 5, check_vma=False)
```

```python
import functools

import jax
import jax.numpy as jnp
from jax import lax
from jax.experimental import pallas as pl
from jax.experimental.pallas import tpu as pltpu
from jax.sharding import PartitionSpec as P

BF16, F32, I32 = jnp.bfloat16, jnp.float32, jnp.int32
WIN = 32
LIST = 4096
COL_ROUNDS, COL_HI, COL_LO = 66, 128, 192


def iota(shape, dim):
    return lax.broadcasted_iota(I32, shape, dim)


def exact_dot(lhs, rhs):
    return jnp.dot(lhs, rhs, precision=lax.Precision.HIGHEST, preferred_element_type=F32)


def mm(lhs, rhs):
    return jnp.dot(lhs, rhs, preferred_element_type=F32)


def mm_nt(lhs, rhs):
    return lax.dot_general(lhs, rhs, (((1,), (1,)), ((), ())), preferred_element_type=F32)


def mm_tn(lhs, rhs):
    return lax.dot_general(lhs, rhs, (((0,), (0,)), ((), ())), preferred_element_type=F32)


def to_column(row):
    wide = jnp.broadcast_to(row, (128, row.shape[1]))
    return jnp.transpose(wide)[:, :1]


def route_kernel(capacity, caps, ids_ref, vslot_ref, tbl_ref, pos_ref):
    blocks = ids_ref.shape[1] // 256
    er = iota((256, 256), 0)
    ec = iota((256, 256), 1)
    upper = jnp.where(er < ec, 1.0, 0.0).astype(BF16)
    carry = jnp.zeros((256, 1), F32)
    for b in range(blocks):
        span = slice(b * 256, (b + 1) * 256)
        oh = jnp.where(er == ids_ref[:, span], 1.0, 0.0)
        cum = mm(oh.astype(BF16), upper) + carry
        pos_ref[:, span] = jnp.sum(oh * cum, axis=0, keepdims=True)
        carry = carry + jnp.sum(oh, axis=1, keepdims=True)
    hot = (er[:, :1] & 63) == 0
    cnt = jnp.where(hot, carry, jnp.minimum(carry, float(capacity)))
    cold_cnt = jnp.broadcast_to(jnp.where(hot, 0.0, cnt), (256, 128))
    dr, dc = er >> 6, ec >> 6
    same = jnp.where(dr == dc, 1.0, 0.0)
    cold_tot = exact_dot(same, cold_cnt)[:, :1]
    rel = exact_dot(jnp.where(ec < er, same, 0.0), cold_cnt)[:, :1]
    rounds = jnp.ones((256, 1), F32)
    for k in range(1, 1 + ids_ref.shape[1] // min(caps)):
        more = (cold_tot > float(k * caps[0])) | (hot & (cnt > float(k * caps[1])))
        rounds = rounds + jnp.where(more, 1.0, 0.0)
    rounds = jnp.max(rounds, axis=0, keepdims=True)
    lm = er & 63
    rel_hi = jnp.floor(rel * 0.0625)
    table = jnp.where((ec == lm) & (lm > 0), cnt, 0.0)
    table += jnp.where(ec == lm + COL_HI, rel_hi, 0.0) + jnp.where(ec == lm + COL_LO, rel - 16.0 * rel_hi, 0.0)
    table += jnp.where((ec == COL_ROUNDS) & (lm == 0), rounds, 0.0)
    pick = jnp.where((iota((8, 256), 1) >> 6) == iota((8, 256), 0), 1.0, 0.0)
    tbl_ref[...] = exact_dot(pick, table)
    start = (dr[:, :1] * LIST).astype(F32) + jnp.where(hot, float(4 * LIST), rel)
    for b in range(blocks):
        span = slice(b * 256, (b + 1) * 256)
        ids = ids_ref[:, span]
        pos = pos_ref[:, span]
        mine = jnp.sum(jnp.where(er == ids, start, 0.0), axis=0, keepdims=True)
        kept = ((ids & 63) == 0) | (pos < float(capacity))
        vslot_ref[:, span] = jnp.where(kept, mine + pos, -1.0).astype(I32)


def pick_rows(sc_ref, vslot_ref, dest, first_list, cap, rows_n):
    row = iota((rows_n, vslot_ref.shape[1]), 0)
    want = row + (first_list + dest) * LIST + sc_ref[0] * cap
    if cap < rows_n:
        want = jnp.where(row < cap, want, -2)
    return jnp.where(want == vslot_ref[...], 1.0, 0.0).astype(BF16)


def add_table(rows, tbl_ref, dest, cap):
    tbl = tbl_ref[pl.ds(dest, 1), :]
    tbl = jnp.concatenate([tbl, jnp.zeros((1, rows.shape[1] - tbl.shape[1]), F32)], axis=1)
    return jnp.where(iota(rows.shape, 0) == cap, tbl, rows)


def pack_x_kernel(offs, cap, sc_ref, vslot_ref, tbl_ref, x_ref, *send_refs):
    for off, send_ref in zip(offs, send_refs):
        dest = sc_ref[1] ^ off
        perm = pick_rows(sc_ref, vslot_ref, dest, 0, cap, send_ref.shape[0])
        send_ref[...] = add_table(mm(perm, x_ref[...]), tbl_ref, dest, cap).astype(BF16)


def pack_g_kernel(offs, cap, sc_ref, vslot_ref, gate_ref, dy_ref, g_ref, *send_refs):
    for b in range(gate_ref.shape[1] // 256):
        span = slice(b * 256, (b + 1) * 256)
        gate = to_column(gate_ref[:, span])
        g_ref[span, :] = (gate * dy_ref[span, :].astype(F32)).astype(BF16)
    for off, send_ref in zip(offs, send_refs):
        perm = pick_rows(sc_ref, vslot_ref, sc_ref[1] ^ off, 0, cap, send_ref.shape[0])
        send_ref[...] = mm(perm, g_ref[...]).astype(BF16)


def pack_xg_kernel(offs, cap, sc_ref, vslot_ref, tbl_ref, x_ref, g_ref, *send_refs):
    n = len(offs)
    for i, off in enumerate(offs):
        dest = sc_ref[1] ^ off
        perm = pick_rows(sc_ref, vslot_ref, dest, 0, cap, send_refs[i].shape[0])
        send_refs[i][...] = add_table(mm(perm, x_ref[...]), tbl_ref, dest, cap).astype(BF16)
        send_refs[n + i][...] = mm(perm, g_ref[...]).astype(BF16)


def pack_hot_kernel(offs, first_list, cap, sc_ref, vslot_ref, x_ref, g_ref, *send_refs):
    d = x_ref.shape[1]
    for off, send_ref in zip(offs, send_refs):
        perm = pick_rows(sc_ref, vslot_ref, sc_ref[1] ^ off, first_list, cap, send_ref.shape[0])
        send_ref[:, :d] = mm(perm, x_ref[...]).astype(BF16)
        send_ref[:, d:] = mm(perm, g_ref[...]).astype(BF16)


def table_kernel(cap, local_n, sc_ref, *refs):
    win_ref, rounds_ref = refs[-2:]
    rounds = jnp.zeros((1, 1), F32)
    for k, ref in enumerate(refs[:-2]):
        head = ref[...].astype(F32)[15:16]
        rel = head[:, COL_HI:COL_HI + local_n] * 16.0 + head[:, COL_LO:COL_LO + local_n] - (sc_ref[0] * cap).astype(F32)
        end = jnp.clip(rel + head[:, :local_n], 0.0, float(cap))
        rel = jnp.clip(rel, 0.0, float(cap))
        win_ref[k:k + 1, :] = jnp.concatenate([end - rel, rel], axis=1).astype(I32)
        rounds = jnp.maximum(rounds, head[:, COL_ROUNDS:COL_ROUNDS + 1])
    rounds_ref[...] = jnp.broadcast_to(rounds, (1, 128)).astype(I32)


def elementwise(a, b, dh):
    a, b, dh = (v.astype(BF16).astype(F32) for v in (a, b, dh))
    s = jax.nn.sigmoid(a)
    silu = a * s
    h = (silu * b).astype(BF16)
    da = (dh * b * (s * (1.0 + a * (1.0 - s)))).astype(BF16)
    db = (dh * silu).astype(BF16)
    return h, da, db


def first_stage(x, g, w1, w3, w2):
    return mm(x, w1), mm(x, w3), mm_nt(g, w2)


def second_stage(h, da, db, w1, w3, w2):
    return mm(h, w2).astype(BF16), (mm_nt(da, w1) + mm_nt(db, w3)).astype(BF16)


def window(tbl_ref, src, expert, rows_n):
    first = tbl_ref[src, 64 + expert]
    base = pl.multiple_of(jnp.minimum((first // 16) * 16, rows_n - WIN), 16)
    return base, first - base, tbl_ref[src, expert]


def load_rows(xg_refs, tbl_ref, expert):
    parts = []
    for src, ref in enumerate(xg_refs):
        base, off, count = window(tbl_ref, src, expert, ref.shape[0])
        rows = ref[pl.ds(base, WIN), :]
        r = iota((WIN, 1), 0)
        parts.append(jnp.where((r >= off) & (r < off + count), rows, jnp.zeros_like(rows)))
    return jnp.concatenate(parts, axis=0)


def cold_kernel(srcs, pair, tbl_ref, *refs):
    x_refs, gy_refs, (w1_ref, w3_ref, w2_ref), *refs = refs[:srcs], refs[srcs:2 * srcs], refs[2 * srcs:2 * srcs + 3], *refs[2 * srcs + 3:]
    od_refs, dab_refs, g2_ref = refs[:srcs], refs[srcs:-1], refs[-1]
    step = pl.program_id(0)
    d, f = w1_ref.shape[1:]

    @pl.when(step == 0)
    def _():
        for ref in od_refs + dab_refs:
            ref[...] = jnp.zeros_like(ref)

    xs = [load_rows(x_refs, tbl_ref, step * pair + k) for k in range(pair)]
    gs = [load_rows(gy_refs, tbl_ref, step * pair + k) for k in range(pair)]
    firsts = [first_stage(xs[k], gs[k], w1_ref[k], w3_ref[k], w2_ref[k]) for k in range(pair)]
    for k in range(pair):
        h, *dab = elementwise(*firsts[k])
        od = second_stage(h, *dab, w1_ref[k], w3_ref[k], w2_ref[k])
        g2_ref[k] = mm_tn(h, gs[k])
        for src in range(srcs):
            at = pl.ds(window(tbl_ref, src, step * pair + k, od_refs[src].shape[0])[0], WIN)
            span = slice(src * WIN, (src + 1) * WIN)
            for j in range(2):
                od_refs[src][at, j * d:(j + 1) * d] += od[j][span]
                dab_refs[src][at, j * f:(j + 1) * f] += dab[j][span]


def grad_kernel(srcs, pair, tbl_ref, *refs):
    x_refs, dab_refs, (g1_ref, g3_ref) = refs[:srcs], refs[srcs:2 * srcs], refs[2 * srcs:]
    step = pl.program_id(0)
    f = g1_ref.shape[2]
    for k in range(pair):
        expert = step * pair + k
        x = load_rows(x_refs, tbl_ref, expert)
        dab = jnp.concatenate([dab_refs[s][pl.ds(window(tbl_ref, s, expert, dab_refs[s].shape[0])[0], WIN), :] for s in range(srcs)], axis=0)
        g13 = mm_tn(x, dab)
        g1_ref[k] = g13[:, :f]
        g3_ref[k] = g13[:, f:]


def hot_weight_kernel(w1_ref, w3_ref, w2_ref, out_ref):
    f = w1_ref.shape[2]
    out_ref[:, :f] = w1_ref[0]
    out_ref[:, f:2 * f] = w3_ref[0]
    for j in range(w2_ref.shape[2] // f):
        out_ref[j * f:(j + 1) * f, 2 * f:] = w2_ref[0, :, j * f:(j + 1) * f]


def hot_kernel(srcs, *refs):
    xg_refs, w_refs, od_refs = refs[:srcs], refs[srcs:2 * srcs], refs[2 * srcs:]
    d = xg_refs[0].shape[1] // 2
    f = w_refs[0].shape[1] // 3
    firsts, weights = [], []
    for xg_ref, w_ref in zip(xg_refs, w_refs):
        w2 = jnp.concatenate([w_ref[j * f:(j + 1) * f, 2 * f:] for j in range(d // f)], axis=1)
        weights.append((w_ref[:, :f], w_ref[:, f:2 * f], w2))
        firsts.append(first_stage(xg_ref[:, :d], xg_ref[:, d:], *weights[-1]))
    for first, weight, od_ref in zip(firsts, weights, od_refs):
        out, dx = second_stage(*elementwise(*first), *weight)
        od_ref[:, :d] = out
        od_ref[:, d:] = dx


def hot_grad_kernel(srcs, *refs):
    xg_refs, (w1_ref, w3_ref, w2_ref), (g1_ref, g3_ref, g2_ref) = refs[:srcs], refs[srcs:srcs + 3], refs[srcs + 6:]
    d = w1_ref.shape[1]
    w1, w3, w2 = w1_ref[0], w3_ref[0], w2_ref[0]
    for k in range(0, srcs, 2):
        xg = jnp.concatenate([xg_refs[k][...], xg_refs[k + 1][...]], axis=0)
        x, g = xg[:, :d], xg[:, d:]
        h, da, db = elementwise(*first_stage(x, g, w1, w3, w2))
        new = mm_tn(x, da), mm_tn(x, db), mm_tn(h, g)
        for ref, val in zip((g1_ref, g3_ref, g2_ref), new):
            ref[0] = ref[0] + val if k else val


def combine_kernel(srcs, caps, sc_ref, vslot_ref, gate_ref, *refs):
    ret_refs, (y_ref, dx_ref, ret_ref, sem) = refs[:-4], refs[-4:]
    d = y_ref.shape[1]

    @pl.when(pl.program_id(0) == 0)
    def _():
        copies, at = [], 0
        for i, ref in enumerate(ret_refs):
            rows = ref.shape[0]
            copies.append(pltpu.make_async_copy(ref, ret_ref.at[pl.ds(at, rows)], sem.at[i]))
            at += rows
        for copy in copies:
            copy.start()
        for copy in copies:
            copy.wait()

    vslot = to_column(vslot_ref[...].astype(F32))
    lane = iota((1, ret_ref.shape[0]), 1)
    have, at = lane, 0
    for i, ref in enumerate(ret_refs):
        kind, off = divmod(i, srcs)
        base = (kind * srcs + (sc_ref[1] ^ off)) * LIST + sc_ref[0] * caps[kind] - at
        have = jnp.where(lane >= at, lane + base, have)
        at += ref.shape[0]
        have = jnp.where((lane >= at - ref.shape[0] + caps[kind]) & (lane < at), -2, have)
    pick = jnp.where(have.astype(F32) == vslot, 1.0, 0.0).astype(BF16)
    y_ref[...] = (to_column(gate_ref[...]) * mm(pick, ret_ref[:, :d])).astype(BF16)
    dx_ref[...] = mm(pick, ret_ref[:, d:]).astype(BF16)


def params(mib):
    return pltpu.CompilerParams(vmem_limit_bytes=mib * 2 ** 20, dimension_semantics=('arbitrary',))


def cost(flops, nbytes):
    return pl.CostEstimate(flops=int(flops), bytes_accessed=int(nbytes), transcendentals=0)


def prefetched(grid, in_specs, out_specs, scratch=()):
    return pltpu.PrefetchScalarGridSpec(num_scalar_prefetch=1, grid=grid, in_specs=in_specs, out_specs=out_specs, scratch_shapes=list(scratch))


COLD_SLAB, COLD_CAP, HOT_SLAB, PAIR = 272, 271, 288, 4


def solution(mesh):
    srcs = mesh.shape['expert']
    tok_spec = P(('data', 'expert'))
    weight_spec = P('expert')
    whole = functools.partial(pl.BlockSpec, pipeline_mode=pl.Buffered(1))
    sds = jax.ShapeDtypeStruct

    def shard_body(tok_x, route_idx, route_gate, grad_y, w_gate, w_up, w_down):
        tok_n, d = tok_x.shape
        local_n, _, f = w_gate.shape
        capacity = max(4, 2 * tok_n // (local_n * srcs))
        ids_row = route_idx.reshape(1, tok_n)
        gate_row = route_gate.reshape(1, tok_n)
        w_bytes = local_n * 3 * d * f * 2
        hot_rows = srcs * HOT_SLAB

        vslot, tbl = pl.pallas_call(
            functools.partial(route_kernel, capacity, (COLD_CAP, HOT_SLAB)),
            out_shape=[sds((1, tok_n), I32), sds((8, 256), F32)],
            scratch_shapes=[pltpu.VMEM((1, tok_n), F32)],
            name='route',
        )(ids_row)
        me = lax.axis_index('expert').astype(I32)
        flat = lambda *_: (0, 0)
        row_spec, tbl_spec, tok_spec_in = whole((1, tok_n), flat), whole((8, 256), flat), whole((tok_n, d), flat)

        def pack(kernel, sc, ins, in_specs, outs, name):
            return pl.pallas_call(
                kernel,
                grid_spec=prefetched((1,), in_specs, [whole(o, flat) for o in outs]),
                out_shape=[sds(o, BF16) for o in outs],
                compiler_params=params(62),
                cost_estimate=cost(2 * sum(o[0] * o[1] for o in outs) * tok_n, 4 * tok_n * d),
                name=name,
            )(sc, *ins)

        def exchange(rows):
            return [rows[0]] + [lax.ppermute(rows[k], 'expert', [(i, i ^ k) for i in range(srcs)]) for k in range(1, srcs)]

        def swap(one):
            send = lambda v, k: lax.ppermute(v, 'expert', [(i, i ^ k) for i in range(srcs)])
            far = send(one, 2)
            return [one, send(one, 1), far, send(far, 1)]

        def combine(sc, rets):
            blk = pl.BlockSpec((256, d), lambda i, t: (i, 0))
            row = pl.BlockSpec((1, 256), lambda i, t: (0, i))
            total = sum(r.shape[0] for r in rets)
            return pl.pallas_call(
                functools.partial(combine_kernel, srcs, (COLD_CAP, HOT_SLAB)),
                grid_spec=prefetched((tok_n // 256,), [row, row] + [pl.BlockSpec(memory_space=pl.ANY)] * len(rets), [blk, blk], [pltpu.VMEM((total, 2 * d), BF16), pltpu.SemaphoreType.DMA((len(rets),))]),
                out_shape=[sds((tok_n, d), BF16), sds((tok_n, d), BF16)],
                compiler_params=params(24),
                cost_estimate=cost(2 * tok_n * total * 2 * d, total * 2 * d * 4),
                name='combine',
            )(sc, vslot, gate_row, *rets)

        def one_round(rnd, pair):
            sc = jnp.concatenate([rnd, me[None]])
            far, near = (2, 3), (0, 1)
            cold, hot = (COLD_SLAB, d), (HOT_SLAB, 2 * d)
            x_far = pack(functools.partial(pack_x_kernel, far, COLD_CAP), sc, (vslot, tbl, tok_x), [row_spec, tbl_spec, tok_spec_in], [cold] * 2, 'pack_x')
            grad_g, *g_far = pack(functools.partial(pack_g_kernel, far, COLD_CAP), sc, (vslot, gate_row, grad_y), [row_spec, row_spec, tok_spec_in], [(tok_n, d)] + [cold] * 2, 'pack_g')
            xg_near = pack(functools.partial(pack_xg_kernel, near, COLD_CAP), sc, (vslot, tbl, tok_x, grad_g), [row_spec, tbl_spec, tok_spec_in, tok_spec_in], [cold] * 4, 'pack_xg')
            cold_x = exchange(list(xg_near[:2]) + list(x_far))
            cold_g = exchange(list(xg_near[2:]) + list(g_far))
            hot_send = []
            for offs in (near, far):
                hot_send += pack(functools.partial(pack_hot_kernel, offs, srcs, HOT_SLAB), sc, (vslot, tok_x, grad_g), [row_spec, tok_spec_in, tok_spec_in], [hot] * 2, 'pack_hot')
            hot_xg = exchange(hot_send)
            last = pl.BlockSpec((16, 256), lambda i, t: (COLD_SLAB // 16 - 1, 0))
            win_tbl, rounds = pl.pallas_call(
                functools.partial(table_kernel, COLD_CAP, local_n),
                grid_spec=prefetched((1,), [last] * srcs, [whole((srcs, 2 * local_n), flat), whole((1, 128), flat)]),
                out_shape=[sds((srcs, 2 * local_n), I32), sds((1, 128), I32)],
                compiler_params=params(62),
                name='table',
            )(sc, *cold_x)

            first = lambda *_: (0, 0, 0)
            any_spec = pl.BlockSpec(memory_space=pl.ANY)
            w13_0, w2_0 = whole((1, d, f), first), whole((1, f, d), first)
            slab_spec = whole((COLD_SLAB, 2 * d), flat)
            x_spec = whole((COLD_SLAB, d), flat)
            dab_spec = whole((COLD_SLAB, 2 * f), flat)
            w13 = pl.BlockSpec((pair, d, f), lambda i, t: (i, 0, 0))
            w2 = pl.BlockSpec((pair, f, d), lambda i, t: (i, 0, 0))
            *res, grad2 = pl.pallas_call(
                functools.partial(cold_kernel, srcs, pair),
                grid_spec=prefetched((local_n // pair,), [x_spec] * (2 * srcs) + [w13, w13, w2], [slab_spec] * srcs + [dab_spec] * srcs + [w2]),
                out_shape=[sds((COLD_SLAB, 2 * d), BF16)] * srcs + [sds((COLD_SLAB, 2 * f), BF16)] * srcs + [sds((local_n, f, d), F32)],
                compiler_params=params(62),
                cost_estimate=cost(2 * 7 * 512 * local_n * d * f, w_bytes),
                name='cold',
            )(win_tbl, *cold_x, *cold_g, w_gate, w_up, w_down)
            cold_od, cold_dab = res[:srcs], res[srcs:]
            cold_ret = exchange(cold_od)

            hot_w = pl.pallas_call(
                hot_weight_kernel,
                grid=(1,),
                in_specs=[w13_0, w13_0, w2_0],
                out_specs=whole((d, 3 * f), flat),
                out_shape=sds((d, 3 * f), BF16),
                compiler_params=params(62),
                name='hot_weight',
            )(w_gate, w_up, w_down)
            hot_w = swap(hot_w)
            hot_spec = whole((HOT_SLAB, 2 * d), flat)
            hot_od = pl.pallas_call(
                functools.partial(hot_kernel, srcs),
                grid=(1,),
                in_specs=[hot_spec] * srcs + [whole((d, 3 * f), flat)] * srcs,
                out_specs=[hot_spec] * srcs,
                out_shape=[sds((HOT_SLAB, 2 * d), BF16)] * srcs,
                compiler_params=params(28),
                cost_estimate=cost(2 * 6 * hot_rows * d * f, 4 * hot_rows * d * 4),
                name='hot',
            )(*hot_send, *hot_w)

            grad1, grad3 = pl.pallas_call(
                functools.partial(grad_kernel, srcs, pair),
                grid_spec=prefetched((local_n // pair,), [x_spec] * srcs + [dab_spec] * srcs, [w13, w13]),
                out_shape=[sds((local_n, d, f), F32)] * 2,
                compiler_params=params(62),
                cost_estimate=cost(2 * 2 * 512 * local_n * d * f, 2 * w_bytes),
                name='grads',
            )(win_tbl, *cold_x, *cold_dab)

            grads = pl.pallas_call(
                functools.partial(hot_grad_kernel, srcs),
                grid=(1,),
                in_specs=[hot_spec] * srcs + [w13_0, w13_0, w2_0] + [any_spec] * 3,
                out_specs=[w13_0, w13_0, w2_0],
                out_shape=[sds((local_n, d, f), F32), sds((local_n, d, f), F32), sds((local_n, f, d), F32)],
                input_output_aliases={srcs + 3: 0, srcs + 4: 1, srcs + 5: 2},
                compiler_params=params(26),
                cost_estimate=cost(2 * 6 * hot_rows * d * f, 4 * hot_rows * d * 4),
                name='hot_grads',
            )(*hot_xg, w_gate, w_up, w_down, grad1, grad3, grad2)

            y, dx = combine(sc, cold_ret + list(hot_od))
            return rounds[0, 0], (y, dx, *grads)

        rounds, outs = one_round(jnp.zeros((1,), I32), PAIR)

        def more(state):
            return state[0][0] < rounds

        def again(state):
            _, extra = one_round(state[0], 1)
            return (state[0] + 1, *(a + b for a, b in zip(state[1:], extra)))

        return lax.while_loop(more, again, (jnp.ones((1,), I32), *outs))[1:]

    return jax.shard_map(shard_body, mesh=mesh, in_specs=(tok_spec, tok_spec, tok_spec, tok_spec, weight_spec, weight_spec, weight_spec), out_specs=(tok_spec,) * 5, check_vma=False)
```

```python
import functools

import jax
import jax.numpy as jnp
from jax import lax
from jax.experimental import pallas as pl
from jax.experimental.pallas import tpu as pltpu
from jax.sharding import PartitionSpec as P


BF16, F32, I32 = jnp.bfloat16, jnp.float32, jnp.int32
WIN = 32
LIST = 4096
COL_ROUNDS, COL_HI, COL_LO = 66, 128, 192


def iota(shape, dim):
    return lax.broadcasted_iota(I32, shape, dim)


def exact_dot(lhs, rhs):
    return jnp.dot(lhs, rhs, precision=lax.Precision.HIGHEST, preferred_element_type=F32)


def mm(lhs, rhs):
    return jnp.dot(lhs, rhs, preferred_element_type=F32)


def mm_nt(lhs, rhs):
    return lax.dot_general(lhs, rhs, (((1,), (1,)), ((), ())), preferred_element_type=F32)


def mm_tn(lhs, rhs):
    return lax.dot_general(lhs, rhs, (((0,), (0,)), ((), ())), preferred_element_type=F32)


def to_column(row):
    wide = jnp.broadcast_to(row, (128, row.shape[1]))
    return jnp.transpose(wide)[:, :1]


def route_kernel(capacity, caps, offs, sc_ref, ids_ref, x_hbm, vslot_ref, tbl_ref, *refs):
    send_refs, (pos_ref, x_ref, sem) = refs[:-3], refs[-3:]
    load = pltpu.make_async_copy(x_hbm, x_ref, sem)
    load.start()
    blocks = ids_ref.shape[1] // 256
    er = iota((256, 256), 0)
    ec = iota((256, 256), 1)
    upper = jnp.where(er < ec, 1.0, 0.0).astype(BF16)
    carry = jnp.zeros((256, 1), F32)
    for b in range(blocks):
        span = slice(b * 256, (b + 1) * 256)
        oh = jnp.where(er == ids_ref[:, span], 1.0, 0.0)
        cum = mm(oh.astype(BF16), upper) + carry
        pos_ref[:, span] = jnp.sum(oh * cum, axis=0, keepdims=True)
        carry = carry + jnp.sum(oh, axis=1, keepdims=True)
    hot = (er[:, :1] & 63) == 0
    cnt = jnp.where(hot, carry, jnp.minimum(carry, float(capacity)))
    cold_cnt = jnp.broadcast_to(jnp.where(hot, 0.0, cnt), (256, 128))
    dr, dc = er >> 6, ec >> 6
    same = jnp.where(dr == dc, 1.0, 0.0)
    cold_tot = exact_dot(same, cold_cnt)[:, :1]
    rel = exact_dot(jnp.where(ec < er, same, 0.0), cold_cnt)[:, :1]
    rounds = jnp.ones((256, 1), F32)
    for k in range(1, 1 + ids_ref.shape[1] // min(caps)):
        more = (cold_tot > float(k * caps[0])) | (hot & (cnt > float(k * caps[1])))
        rounds = rounds + jnp.where(more, 1.0, 0.0)
    rounds = jnp.max(rounds, axis=0, keepdims=True)
    lm = er & 63
    rel_hi = jnp.floor(rel * 0.0625)
    table = jnp.where((ec == lm) & (lm > 0), cnt, 0.0)
    table += jnp.where(ec == lm + COL_HI, rel_hi, 0.0) + jnp.where(ec == lm + COL_LO, rel - 16.0 * rel_hi, 0.0)
    table += jnp.where((ec == COL_ROUNDS) & (lm == 0), rounds, 0.0)
    pick = jnp.where((iota((8, 256), 1) >> 6) == iota((8, 256), 0), 1.0, 0.0)
    tbl_ref[...] = exact_dot(pick, table)
    start = (dr[:, :1] * LIST).astype(F32) + jnp.where(hot, float(4 * LIST), rel)
    for b in range(blocks):
        span = slice(b * 256, (b + 1) * 256)
        ids = ids_ref[:, span]
        pos = pos_ref[:, span]
        mine = jnp.sum(jnp.where(er == ids, start, 0.0), axis=0, keepdims=True)
        kept = ((ids & 63) == 0) | (pos < float(capacity))
        vslot_ref[:, span] = jnp.where(kept, mine + pos, -1.0).astype(I32)
    load.wait()
    for off, send_ref in zip(offs, send_refs):
        dest = sc_ref[1] ^ off
        perm = pick_rows(sc_ref, vslot_ref, dest, 0, caps[0], send_ref.shape[0])
        send_ref[...] = add_table(mm(perm, x_ref[...]), tbl_ref, dest, caps[0]).astype(BF16)


def pick_rows(sc_ref, vslot_ref, dest, first_list, cap, rows_n):
    row = iota((rows_n, vslot_ref.shape[1]), 0)
    want = row + (first_list + dest) * LIST + sc_ref[0] * cap
    if cap < rows_n:
        want = jnp.where(row < cap, want, -2)
    return jnp.where(want == vslot_ref[...], 1.0, 0.0).astype(BF16)


def add_table(rows, tbl_ref, dest, cap):
    tbl = tbl_ref[pl.ds(dest, 1), :]
    tbl = jnp.concatenate([tbl, jnp.zeros((1, rows.shape[1] - tbl.shape[1]), F32)], axis=1)
    return jnp.where(iota(rows.shape, 0) == cap, tbl, rows)


def pack_g_kernel(offs, cap, sc_ref, vslot_ref, gate_ref, dy_ref, g_ref, *send_refs):
    for b in range(gate_ref.shape[1] // 256):
        span = slice(b * 256, (b + 1) * 256)
        gate = to_column(gate_ref[:, span])
        g_ref[span, :] = (gate * dy_ref[span, :].astype(F32)).astype(BF16)
    for off, send_ref in zip(offs, send_refs):
        perm = pick_rows(sc_ref, vslot_ref, sc_ref[1] ^ off, 0, cap, send_ref.shape[0])
        send_ref[...] = mm(perm, g_ref[...]).astype(BF16)


def pack_rest_kernel(offs, srcs, caps, sc_ref, vslot_ref, tbl_ref, x_ref, g_ref, *send_refs):
    n, d = len(offs), x_ref.shape[1]
    for i, off in enumerate(offs):
        dest = sc_ref[1] ^ off
        perm = pick_rows(sc_ref, vslot_ref, dest, 0, caps[0], send_refs[i].shape[0])
        send_refs[i][...] = add_table(mm(perm, x_ref[...]), tbl_ref, dest, caps[0]).astype(BF16)
        send_refs[n + i][...] = mm(perm, g_ref[...]).astype(BF16)
    for off, send_ref in enumerate(send_refs[2 * n:]):
        perm = pick_rows(sc_ref, vslot_ref, sc_ref[1] ^ off, srcs, caps[1], send_ref.shape[0])
        send_ref[:, :d] = mm(perm, x_ref[...]).astype(BF16)
        send_ref[:, d:] = mm(perm, g_ref[...]).astype(BF16)


def table_kernel(cap, local_n, sc_ref, *refs):
    win_ref, rounds_ref = refs[-2:]
    rounds = jnp.zeros((1, 1), F32)
    for k, ref in enumerate(refs[:-2]):
        head = ref[...].astype(F32)[15:16]
        rel = head[:, COL_HI:COL_HI + local_n] * 16.0 + head[:, COL_LO:COL_LO + local_n] - (sc_ref[0] * cap).astype(F32)
        end = jnp.clip(rel + head[:, :local_n], 0.0, float(cap))
        rel = jnp.clip(rel, 0.0, float(cap))
        win_ref[k:k + 1, :] = jnp.concatenate([end - rel, rel], axis=1).astype(I32)
        rounds = jnp.maximum(rounds, head[:, COL_ROUNDS:COL_ROUNDS + 1])
    rounds_ref[...] = jnp.broadcast_to(rounds, (1, 128)).astype(I32)


def elementwise(a, b, dh):
    a, b, dh = (v.astype(BF16).astype(F32) for v in (a, b, dh))
    s = jax.nn.sigmoid(a)
    silu = a * s
    h = (silu * b).astype(BF16)
    da = (dh * b * (s * (1.0 + a * (1.0 - s)))).astype(BF16)
    db = (dh * silu).astype(BF16)
    return h, da, db


def first_stage(x, g, w1, w3, w2):
    return mm(x, w1), mm(x, w3), mm_nt(g, w2)


def second_stage(h, da, db, w1, w3, w2):
    return mm(h, w2).astype(BF16), jnp.transpose(mm_nt(w1, da) + mm_nt(w3, db)).astype(BF16)


def window(tbl_ref, src, expert, rows_n):
    first = tbl_ref[src, 64 + expert]
    base = pl.multiple_of(jnp.minimum((first // 16) * 16, rows_n - WIN), 16)
    return base, first - base, tbl_ref[src, expert]


def load_rows(xg_refs, tbl_ref, expert):
    parts = []
    for src, ref in enumerate(xg_refs):
        base, off, count = window(tbl_ref, src, expert, ref.shape[0])
        rows = ref[pl.ds(base, WIN), :]
        r = iota((WIN, 1), 0)
        parts.append(jnp.where((r >= off) & (r < off + count), rows, jnp.zeros_like(rows)))
    return jnp.concatenate(parts, axis=0)


def cold_kernel(srcs, pair, tbl_ref, *refs):
    x_refs, gy_refs, (w1_ref, w3_ref, w2_ref), *refs = refs[:srcs], refs[srcs:2 * srcs], refs[2 * srcs:2 * srcs + 3], *refs[2 * srcs + 3:]
    od_refs, dab_refs, g2_ref = refs[:srcs], refs[srcs:-1], refs[-1]
    step = pl.program_id(0)
    d, f = w1_ref.shape[1:]

    @pl.when(step == 0)
    def _():
        for ref in od_refs + dab_refs:
            ref[...] = jnp.zeros_like(ref)

    xs = [load_rows(x_refs, tbl_ref, step * pair + k) for k in range(pair)]
    gs = [load_rows(gy_refs, tbl_ref, step * pair + k) for k in range(pair)]
    firsts = [first_stage(xs[k], gs[k], w1_ref[k], w3_ref[k], w2_ref[k]) for k in range(pair)]
    for k in range(pair):
        h, *dab = elementwise(*firsts[k])
        od = second_stage(h, *dab, w1_ref[k], w3_ref[k], w2_ref[k])
        g2_ref[k] = mm_tn(h, gs[k])
        for src in range(srcs):
            at = pl.ds(window(tbl_ref, src, step * pair + k, od_refs[src].shape[0])[0], WIN)
            span = slice(src * WIN, (src + 1) * WIN)
            for j in range(2):
                od_refs[src][at, j * d:(j + 1) * d] += od[j][span]
                dab_refs[src][at, j * f:(j + 1) * f] += dab[j][span]


def grad_kernel(srcs, pair, tbl_ref, *refs):
    x_refs, dab_refs, hot_refs, w_refs, refs = refs[:srcs], refs[srcs:2 * srcs], refs[2 * srcs:3 * srcs], refs[3 * srcs:4 * srcs], refs[4 * srcs:]
    (g1_ref, g3_ref), od_refs, (hot_buf, w_buf, od_buf, in_sem, out_sem) = refs[:2], refs[2:2 + srcs], refs[2 + srcs:]
    step, steps = pl.program_id(0), pl.num_programs(0)
    _, f = g1_ref.shape[1:]

    def loads(k):
        return [pltpu.make_async_copy(hot_refs[k], hot_buf.at[k], in_sem.at[2 * k]), pltpu.make_async_copy(w_refs[k], w_buf.at[k], in_sem.at[2 * k + 1])]

    def store(k):
        return pltpu.make_async_copy(od_buf.at[k], od_refs[k], out_sem.at[k])

    @pl.when(step == 0)
    def _():
        for k in range(srcs):
            for copy in loads(k):
                copy.start()

    for k in range(srcs):
        @pl.when(step == 2 + 2 * k)
        def _(k=k):
            for copy in loads(k):
                copy.wait()
            hot_rows(hot_buf.at[k], w_buf.at[k], od_buf.at[k])
            store(k).start()

    for k in range(pair):
        expert = step * pair + k
        x = load_rows(x_refs, tbl_ref, expert)
        dab = jnp.concatenate([dab_refs[s][pl.ds(window(tbl_ref, s, expert, dab_refs[s].shape[0])[0], WIN), :] for s in range(srcs)], axis=0)
        g13 = mm_tn(x, dab)
        g1_ref[k] = g13[:, :f]
        g3_ref[k] = g13[:, f:]

    @pl.when(step == steps - 1)
    def _():
        for k in range(srcs):
            store(k).wait()


def hot_weight_kernel(w1_ref, w3_ref, w2_ref, after_ref, out_ref):
    del after_ref
    f = w1_ref.shape[2]
    out_ref[:, :f] = w1_ref[0]
    out_ref[:, f:2 * f] = w3_ref[0]
    for j in range(w2_ref.shape[2] // f):
        out_ref[j * f:(j + 1) * f, 2 * f:] = w2_ref[0, :, j * f:(j + 1) * f]


def hot_rows(xg_ref, w_ref, od_ref):
    d = xg_ref.shape[1] // 2
    f = w_ref.shape[1] // 3
    w1, w3 = w_ref[:, :f], w_ref[:, f:2 * f]
    w2 = jnp.concatenate([w_ref[j * f:(j + 1) * f, 2 * f:] for j in range(d // f)], axis=1)
    out, dx = second_stage(*elementwise(*first_stage(xg_ref[:, :d], xg_ref[:, d:], w1, w3, w2)), w1, w3, w2)
    od_ref[:, :d] = out
    od_ref[:, d:] = dx


def hot_grad_kernel(srcs, *refs):
    xg_refs, (w1_ref, w3_ref, w2_ref), (g1_ref, g3_ref, g2_ref) = refs[:srcs], refs[srcs:srcs + 3], refs[srcs + 6:]
    d = w1_ref.shape[1]
    w1, w3, w2 = w1_ref[0], w3_ref[0], w2_ref[0]
    for k in range(0, srcs, 2):
        xg = jnp.concatenate([xg_refs[k][...], xg_refs[k + 1][...]], axis=0)
        x, g = xg[:, :d], xg[:, d:]
        h, da, db = elementwise(*first_stage(x, g, w1, w3, w2))
        new = mm_tn(x, da), mm_tn(x, db), mm_tn(h, g)
        for ref, val in zip((g1_ref, g3_ref, g2_ref), new):
            ref[0] = ref[0] + val if k else val


def combine_kernel(srcs, caps, sc_ref, vslot_ref, gate_ref, *refs):
    ret_refs, (y_ref, dx_ref, ret_ref, sem) = refs[:-4], refs[-4:]
    d = y_ref.shape[1]

    @pl.when(pl.program_id(0) == 0)
    def _():
        copies, at = [], 0
        for i, ref in enumerate(ret_refs):
            rows = ref.shape[0]
            copies.append(pltpu.make_async_copy(ref, ret_ref.at[pl.ds(at, rows)], sem.at[i]))
            at += rows
        for copy in copies:
            copy.start()
        for copy in copies:
            copy.wait()

    vslot = to_column(vslot_ref[...].astype(F32))
    lane = iota((1, ret_ref.shape[0]), 1)
    have, at = lane, 0
    for i, ref in enumerate(ret_refs):
        kind, off = divmod(i, srcs)
        base = (kind * srcs + (sc_ref[1] ^ off)) * LIST + sc_ref[0] * caps[kind] - at
        have = jnp.where(lane >= at, lane + base, have)
        at += ref.shape[0]
        have = jnp.where((lane >= at - ref.shape[0] + caps[kind]) & (lane < at), -2, have)
    pick = jnp.where(have.astype(F32) == vslot, 1.0, 0.0).astype(BF16)
    y_ref[...] = (to_column(gate_ref[...]) * mm(pick, ret_ref[:, :d])).astype(BF16)
    dx_ref[...] = mm(pick, ret_ref[:, d:]).astype(BF16)


def kernel_call(body, **options):
    return pl.pallas_call(body, **options)


def params(mib):
    return pltpu.CompilerParams(vmem_limit_bytes=mib * 2 ** 20, dimension_semantics=('arbitrary',))


def cost(flops, nbytes):
    return pl.CostEstimate(flops=int(flops), bytes_accessed=int(nbytes), transcendentals=0)


def prefetched(grid, in_specs, out_specs, scratch=()):
    return pltpu.PrefetchScalarGridSpec(num_scalar_prefetch=1, grid=grid, in_specs=in_specs, out_specs=out_specs, scratch_shapes=list(scratch))


COLD_SLAB, COLD_CAP, HOT_SLAB, PAIR, COLD_PAIR = 272, 271, 288, 4, 8


def solution(mesh):
    srcs = mesh.shape['expert']
    tok_spec = P(('data', 'expert'))
    weight_spec = P('expert')
    whole = functools.partial(pl.BlockSpec, pipeline_mode=pl.Buffered(1))
    sds = jax.ShapeDtypeStruct

    def shard_body(tok_x, route_idx, route_gate, grad_y, w_gate, w_up, w_down):
        tok_n, d = tok_x.shape
        local_n, _, f = w_gate.shape
        capacity = max(4, 2 * tok_n // (local_n * srcs))
        ids_row = route_idx.reshape(1, tok_n)
        gate_row = route_gate.reshape(1, tok_n)
        w_bytes = local_n * 3 * d * f * 2
        hot_rows = srcs * HOT_SLAB

        me = lax.axis_index('expert').astype(I32)
        flat = lambda *_: (0, 0)
        row_spec, tbl_spec, tok_spec_in = whole((1, tok_n), flat), whole((8, 256), flat), whole((tok_n, d), flat)

        def pack(kernel, sc, ins, in_specs, outs, name):
            return kernel_call(
                kernel,
                grid_spec=prefetched((1,), in_specs, [whole(o, flat) for o in outs]),
                out_shape=[sds(o, BF16) for o in outs],
                compiler_params=params(62),
                cost_estimate=cost(2 * sum(o[0] * o[1] for o in outs) * tok_n, 4 * tok_n * d),
                name=name,
            )(sc, *ins)

        def send(value, k):
            return lax.ppermute(value, 'expert', [(i, i ^ k) for i in range(srcs)])

        def exchange(rows):
            return [rows[0]] + [send(rows[k], k) for k in range(1, srcs)]

        def swap(one):
            far = send(one, 2)
            return [one, send(one, 1), far, send(far, 1)]

        def combine(sc, vslot, rets):
            blk = pl.BlockSpec((256, d), lambda i, t: (i, 0))
            row = pl.BlockSpec((1, 256), lambda i, t: (0, i))
            total = sum(r.shape[0] for r in rets)
            return kernel_call(
                functools.partial(combine_kernel, srcs, (COLD_CAP, HOT_SLAB)),
                grid_spec=prefetched((tok_n // 256,), [row, row] + [pl.BlockSpec(memory_space=pl.ANY)] * len(rets), [blk, blk], [pltpu.VMEM((total, 2 * d), BF16), pltpu.SemaphoreType.DMA((len(rets),))]),
                out_shape=[sds((tok_n, d), BF16), sds((tok_n, d), BF16)],
                compiler_params=params(24),
                cost_estimate=cost(2 * tok_n * total * 2 * d, total * 2 * d * 4),
                name='combine',
            )(sc, vslot, gate_row, *rets)

        def one_round(rnd, pair, wide):
            sc = jnp.concatenate([rnd, me[None]])
            far, near = (2, 3), (0, 1)
            cold, hot = (COLD_SLAB, d), (HOT_SLAB, 2 * d)
            any_spec = pl.BlockSpec(memory_space=pl.ANY)
            caps = (COLD_CAP, HOT_SLAB)
            vslot, tbl, *x_far = kernel_call(
                functools.partial(route_kernel, capacity, caps, far),
                grid_spec=prefetched((1,), [row_spec, any_spec], [row_spec, tbl_spec] + [whole(cold, flat)] * 2, [pltpu.VMEM((1, tok_n), F32), pltpu.VMEM((tok_n, d), BF16), pltpu.SemaphoreType.DMA(())]),
                out_shape=[sds((1, tok_n), I32), sds((8, 256), F32)] + [sds(cold, BF16)] * 2,
                compiler_params=params(62),
                cost_estimate=cost(2 * 2 * COLD_SLAB * d * tok_n, 4 * tok_n * d),
                name='route',
            )(sc, ids_row, tok_x)
            grad_g, *g_far = pack(functools.partial(pack_g_kernel, far, COLD_CAP), sc, (vslot, gate_row, grad_y), [row_spec, row_spec, tok_spec_in], [(tok_n, d)] + [cold] * 2, 'pack_g')
            rest = pack(functools.partial(pack_rest_kernel, near, srcs, caps), sc, (vslot, tbl, tok_x, grad_g), [row_spec, tbl_spec, tok_spec_in, tok_spec_in], [cold] * 4 + [hot] * srcs, 'pack_rest')
            cold_x = exchange(list(rest[:2]) + list(x_far))
            cold_g = exchange(list(rest[2:4]) + list(g_far))
            hot_send = list(rest[4:])
            hot_xg = exchange(hot_send)
            last = pl.BlockSpec((16, 256), lambda i, t: (COLD_SLAB // 16 - 1, 0))
            win_tbl, rounds = kernel_call(
                functools.partial(table_kernel, COLD_CAP, local_n),
                grid_spec=prefetched((1,), [last] * srcs, [whole((srcs, 2 * local_n), flat), whole((1, 128), flat)]),
                out_shape=[sds((srcs, 2 * local_n), I32), sds((1, 128), I32)],
                compiler_params=params(62),
                name='table',
            )(sc, *cold_x)

            first = lambda *_: (0, 0, 0)
            w13_0, w2_0 = whole((1, d, f), first), whole((1, f, d), first)
            slab_spec = whole((COLD_SLAB, 2 * d), flat)
            x_spec = whole((COLD_SLAB, d), flat)
            dab_spec = whole((COLD_SLAB, 2 * f), flat)
            w13 = pl.BlockSpec((pair, d, f), lambda i, t: (i, 0, 0))
            w2 = pl.BlockSpec((pair, f, d), lambda i, t: (i, 0, 0))
            wide_w = [pl.BlockSpec((wide, d, f), lambda i, t: (i, 0, 0))] * 2 + [pl.BlockSpec((wide, f, d), lambda i, t: (i, 0, 0))]
            *res, grad2 = kernel_call(
                functools.partial(cold_kernel, srcs, wide),
                grid_spec=prefetched((local_n // wide,), [x_spec] * (2 * srcs) + [*wide_w], [slab_spec] * srcs + [dab_spec] * srcs + wide_w[2:]),
                out_shape=[sds((COLD_SLAB, 2 * d), BF16)] * srcs + [sds((COLD_SLAB, 2 * f), BF16)] * srcs + [sds((local_n, f, d), F32)],
                compiler_params=params(62),
                cost_estimate=cost(2 * 7 * 512 * local_n * d * f, w_bytes),
                name='cold',
            )(win_tbl, *cold_x, *cold_g, w_gate, w_up, w_down)
            cold_od, cold_dab = res[:srcs], res[srcs:]
            cold_ret = exchange(cold_od)

            hot_w = kernel_call(
                hot_weight_kernel,
                grid=(1,),
                in_specs=[w13_0, w13_0, w2_0, whole((16, 128), flat)],
                out_specs=whole((d, 3 * f), flat),
                out_shape=sds((d, 3 * f), BF16),
                compiler_params=params(62),
                name='hot_weight',
            )(w_gate, w_up, w_down, hot_send[0])
            hot_w = swap(hot_w)
            hot_spec = whole((HOT_SLAB, 2 * d), flat)
            grad1, grad3, *hot_od = kernel_call(
                functools.partial(grad_kernel, srcs, pair),
                grid_spec=prefetched(
                    (local_n // pair,),
                    [x_spec] * srcs + [dab_spec] * srcs + [any_spec] * (2 * srcs),
                    [w13, w13] + [any_spec] * srcs,
                    [pltpu.VMEM((srcs, HOT_SLAB, 2 * d), BF16), pltpu.VMEM((srcs, d, 3 * f), BF16), pltpu.VMEM((srcs, HOT_SLAB, 2 * d), BF16), pltpu.SemaphoreType.DMA((2 * srcs,)), pltpu.SemaphoreType.DMA((srcs,))],
                ),
                out_shape=[sds((local_n, d, f), F32)] * 2 + [sds((HOT_SLAB, 2 * d), BF16)] * srcs,
                compiler_params=params(62),
                cost_estimate=cost(2 * 2 * 512 * local_n * d * f, 2 * w_bytes),
                name='grads',
            )(win_tbl, *cold_x, *cold_dab, *hot_send, *hot_w)

            grads = kernel_call(
                functools.partial(hot_grad_kernel, srcs),
                grid=(1,),
                in_specs=[hot_spec] * srcs + [w13_0, w13_0, w2_0] + [any_spec] * 3,
                out_specs=[w13_0, w13_0, w2_0],
                out_shape=[sds((local_n, d, f), F32), sds((local_n, d, f), F32), sds((local_n, f, d), F32)],
                input_output_aliases={srcs + 3: 0, srcs + 4: 1, srcs + 5: 2},
                compiler_params=params(26),
                cost_estimate=cost(2 * 6 * hot_rows * d * f, 4 * hot_rows * d * 4),
                name='hot_grads',
            )(*hot_xg, w_gate, w_up, w_down, grad1, grad3, grad2)

            y, dx = combine(sc, vslot, cold_ret + list(hot_od))
            return rounds[0, 0], (y, dx, *grads)

        rounds, outs = one_round(jnp.zeros((1,), I32), PAIR, COLD_PAIR)

        def more(state):
            return state[0][0] < rounds

        def again(state):
            _, extra = one_round(state[0], 1, 1)
            return (state[0] + 1, *(a + b for a, b in zip(state[1:], extra)))

        return lax.while_loop(more, again, (jnp.ones((1,), I32), *outs))[1:]

    return jax.shard_map(shard_body, mesh=mesh, in_specs=(tok_spec, tok_spec, tok_spec, tok_spec, weight_spec, weight_spec, weight_spec), out_specs=(tok_spec,) * 5, check_vma=False)
```

```python
import functools

import jax
import jax.numpy as jnp
from jax import lax
from jax.experimental import pallas as pl
from jax.experimental.pallas import tpu as pltpu
from jax.sharding import PartitionSpec as P


BF16, F32, I32 = jnp.bfloat16, jnp.float32, jnp.int32
WIN = 32
LIST, CHUNK = 4096, 512
COL_ROUNDS, COL_HI, COL_LO = 66, 128, 192


def iota(shape, dim):
    return lax.broadcasted_iota(I32, shape, dim)


def exact_dot(lhs, rhs):
    return jnp.dot(lhs, rhs, precision=lax.Precision.HIGHEST, preferred_element_type=F32)


def mm(lhs, rhs):
    return jnp.dot(lhs, rhs, preferred_element_type=F32)


def mm_nt(lhs, rhs):
    return lax.dot_general(lhs, rhs, (((1,), (1,)), ((), ())), preferred_element_type=F32)


def mm_tn(lhs, rhs):
    return lax.dot_general(lhs, rhs, (((0,), (0,)), ((), ())), preferred_element_type=F32)


def to_column(row):
    wide = jnp.broadcast_to(row, (128, row.shape[1]))
    return jnp.transpose(wide)[:, :1]


def route_kernel(capacity, caps, offs, sc_ref, ids_ref, x_hbm, vslot_ref, tbl_ref, *refs):
    send_refs, (pos_ref, x_ref, sem) = refs[:-3], refs[-3:]
    load = pltpu.make_async_copy(x_hbm, x_ref, sem)
    load.start()
    blocks = ids_ref.shape[1] // 256
    er = iota((256, 256), 0)
    ec = iota((256, 256), 1)
    upper = jnp.where(er < ec, 1.0, 0.0).astype(BF16)
    carry = jnp.zeros((256, 1), F32)
    for b in range(blocks):
        span = slice(b * 256, (b + 1) * 256)
        oh = jnp.where(er == ids_ref[:, span], 1.0, 0.0)
        cum = mm(oh.astype(BF16), upper) + carry
        pos_ref[:, span] = jnp.sum(oh * cum, axis=0, keepdims=True)
        carry = carry + jnp.sum(oh, axis=1, keepdims=True)
    hot = (er[:, :1] & 63) == 0
    cnt = jnp.where(hot, carry, jnp.minimum(carry, float(capacity)))
    cold_cnt = jnp.broadcast_to(jnp.where(hot, 0.0, cnt), (256, 128))
    dr, dc = er >> 6, ec >> 6
    same = jnp.where(dr == dc, 1.0, 0.0)
    cold_tot = exact_dot(same, cold_cnt)[:, :1]
    rel = exact_dot(jnp.where(ec < er, same, 0.0), cold_cnt)[:, :1]
    rounds = jnp.ones((256, 1), F32)
    for k in range(1, 1 + ids_ref.shape[1] // min(caps)):
        more = (cold_tot > float(k * caps[0])) | (hot & (cnt > float(k * caps[1])))
        rounds = rounds + jnp.where(more, 1.0, 0.0)
    rounds = jnp.max(rounds, axis=0, keepdims=True)
    lm = er & 63
    rel_hi = jnp.floor(rel * 0.0625)
    table = jnp.where((ec == lm) & (lm > 0), cnt, 0.0)
    table += jnp.where(ec == lm + COL_HI, rel_hi, 0.0) + jnp.where(ec == lm + COL_LO, rel - 16.0 * rel_hi, 0.0)
    table += jnp.where((ec == COL_ROUNDS) & (lm == 0), rounds, 0.0)
    pick = jnp.where((iota((8, 256), 1) >> 6) == iota((8, 256), 0), 1.0, 0.0)
    tbl_ref[...] = exact_dot(pick, table)
    start = (dr[:, :1] * LIST).astype(F32) + jnp.where(hot, float(4 * LIST), rel)
    for b in range(blocks):
        span = slice(b * 256, (b + 1) * 256)
        ids = ids_ref[:, span]
        pos = pos_ref[:, span]
        mine = jnp.sum(jnp.where(er == ids, start, 0.0), axis=0, keepdims=True)
        kept = ((ids & 63) == 0) | (pos < float(capacity))
        vslot_ref[:, span] = jnp.where(kept, mine + pos, -1.0).astype(I32)
    load.wait()
    for off, send_ref in zip(offs, send_refs):
        dest = sc_ref[1] ^ off
        perm = pick_rows(sc_ref, vslot_ref, dest, 0, caps[0], send_ref.shape[0])
        send_ref[...] = add_table(mm(perm, x_ref[...]), tbl_ref, dest, caps[0]).astype(BF16)


def pick_rows(sc_ref, vslot_ref, dest, first_list, cap, rows_n):
    row = iota((rows_n, vslot_ref.shape[1]), 0)
    want = row + (first_list + dest) * LIST + sc_ref[0] * cap
    if cap < rows_n:
        want = jnp.where(row < cap, want, -2)
    return jnp.where(want == vslot_ref[...], 1.0, 0.0).astype(BF16)


def add_table(rows, tbl_ref, dest, cap):
    tbl = tbl_ref[pl.ds(dest, 1), :]
    tbl = jnp.concatenate([tbl, jnp.zeros((1, rows.shape[1] - tbl.shape[1]), F32)], axis=1)
    return jnp.where(iota(rows.shape, 0) == cap, tbl, rows)


def pack_g_kernel(offs, cap, sc_ref, vslot_ref, gate_ref, dy_ref, g_ref, *refs):
    send_refs, acc_ref = refs[:-1], refs[-1]
    for b in range(gate_ref.shape[1] // 256):
        span = slice(b * 256, (b + 1) * 256)
        gate = to_column(gate_ref[:, span])
        g_ref[span, :] = (gate * dy_ref[span, :].astype(F32)).astype(BF16)
    for off, send_ref in zip(offs, send_refs):
        row = iota((send_ref.shape[0], CHUNK), 0)
        want = jnp.where(row < cap, row + (sc_ref[1] ^ off) * LIST + sc_ref[0] * cap, -2)
        gather_rows(acc_ref, send_ref.shape[0], want, vslot_ref, (g_ref,))
        send_ref[...] = acc_ref[...].astype(BF16)


def gather_rows(acc_ref, rows_n, want, vslot_ref, srcs):
    d = srcs[0].shape[1]
    acc_ref[...] = jnp.zeros_like(acc_ref)

    def add(b, _):
        span = pl.ds(pl.multiple_of(b * CHUNK, CHUNK), CHUNK)
        perm = jnp.where(want == vslot_ref[:, span], 1.0, 0.0).astype(BF16)
        for j, ref in enumerate(srcs):
            acc_ref[:rows_n, j * d:(j + 1) * d] += mm(perm, ref[span, :])
        return 0

    lax.fori_loop(0, srcs[0].shape[0] // CHUNK, add, 0)


def pack_rest_kernel(offs, srcs, caps, sc_ref, vslot_ref, tbl_ref, x_ref, g_ref, *refs):
    send_refs, acc_ref = refs[:-1], refs[-1]
    n, d = len(offs), x_ref.shape[1]
    for i, off in enumerate(offs):
        dest = sc_ref[1] ^ off
        rows_n = send_refs[i].shape[0]
        row = iota((rows_n, CHUNK), 0)
        want = jnp.where(row < caps[0], row + dest * LIST + sc_ref[0] * caps[0], -2)
        gather_rows(acc_ref, rows_n, want, vslot_ref, (x_ref, g_ref))
        send_refs[i][...] = add_table(acc_ref[:rows_n, :d], tbl_ref, dest, caps[0]).astype(BF16)
        send_refs[n + i][...] = acc_ref[:rows_n, d:].astype(BF16)
    for off, send_ref in enumerate(send_refs[2 * n:]):
        rows_n = send_ref.shape[0]
        want = iota((rows_n, CHUNK), 0) + (srcs + (sc_ref[1] ^ off)) * LIST + sc_ref[0] * caps[1]
        gather_rows(acc_ref, rows_n, want, vslot_ref, (x_ref, g_ref))
        send_ref[...] = acc_ref[:rows_n, :].astype(BF16)


def table_kernel(cap, local_n, sc_ref, *refs):
    win_ref, rounds_ref = refs[-2:]
    rounds = jnp.zeros((1, 1), F32)
    for k, ref in enumerate(refs[:-2]):
        head = ref[...].astype(F32)[15:16]
        rel = head[:, COL_HI:COL_HI + local_n] * 16.0 + head[:, COL_LO:COL_LO + local_n] - (sc_ref[0] * cap).astype(F32)
        end = jnp.clip(rel + head[:, :local_n], 0.0, float(cap))
        rel = jnp.clip(rel, 0.0, float(cap))
        win_ref[k:k + 1, :] = jnp.concatenate([end - rel, rel], axis=1).astype(I32)
        rounds = jnp.maximum(rounds, head[:, COL_ROUNDS:COL_ROUNDS + 1])
    rounds_ref[...] = jnp.broadcast_to(rounds, (1, 128)).astype(I32)


def elementwise(a, b, dh):
    a, b, dh = (v.astype(BF16).astype(F32) for v in (a, b, dh))
    s = jax.nn.sigmoid(a)
    silu = a * s
    h = (silu * b).astype(BF16)
    da = (dh * b * (s * (1.0 + a * (1.0 - s)))).astype(BF16)
    db = (dh * silu).astype(BF16)
    return h, da, db


def first_stage(x, g, w1, w3, w2):
    return mm(x, w1), mm(x, w3), mm_nt(g, w2)


def second_stage(h, da, db, w1, w3, w2):
    return mm(h, w2).astype(BF16), jnp.transpose(mm_nt(w1, da) + mm_nt(w3, db)).astype(BF16)


def window(tbl_ref, src, expert, rows_n):
    first = tbl_ref[src, 64 + expert]
    base = pl.multiple_of(jnp.minimum((first // 16) * 16, rows_n - WIN), 16)
    return base, first - base, tbl_ref[src, expert]


def load_rows(xg_refs, tbl_ref, expert):
    parts = []
    for src, ref in enumerate(xg_refs):
        base, off, count = window(tbl_ref, src, expert, ref.shape[0])
        rows = ref[pl.ds(base, WIN), :]
        r = iota((WIN, 1), 0)
        parts.append(jnp.where((r >= off) & (r < off + count), rows, jnp.zeros_like(rows)))
    return jnp.concatenate(parts, axis=0)


def cold_kernel(srcs, pair, tbl_ref, *refs):
    x_refs, gy_refs, (w1_ref, w3_ref, w2_ref), *refs = refs[:srcs], refs[srcs:2 * srcs], refs[2 * srcs:2 * srcs + 3], *refs[2 * srcs + 3:]
    od_refs, dab_refs, g2_ref = refs[:srcs], refs[srcs:-1], refs[-1]
    step = pl.program_id(0)
    d, f = w1_ref.shape[1:]

    @pl.when(step == 0)
    def _():
        for ref in od_refs + dab_refs:
            ref[...] = jnp.zeros_like(ref)

    xs = [load_rows(x_refs, tbl_ref, step * pair + k) for k in range(pair)]
    gs = [load_rows(gy_refs, tbl_ref, step * pair + k) for k in range(pair)]
    firsts = [first_stage(xs[k], gs[k], w1_ref[k], w3_ref[k], w2_ref[k]) for k in range(pair)]
    for k in range(pair):
        h, *dab = elementwise(*firsts[k])
        od = second_stage(h, *dab, w1_ref[k], w3_ref[k], w2_ref[k])
        g2_ref[k] = mm_tn(h, gs[k])
        for src in range(srcs):
            at = pl.ds(window(tbl_ref, src, step * pair + k, od_refs[src].shape[0])[0], WIN)
            span = slice(src * WIN, (src + 1) * WIN)
            for j in range(2):
                od_refs[src][at, j * d:(j + 1) * d] += od[j][span]
                dab_refs[src][at, j * f:(j + 1) * f] += dab[j][span]


def grad_kernel(srcs, pair, tbl_ref, *refs):
    x_refs, dab_refs, hot_refs, w_refs, refs = refs[:srcs], refs[srcs:2 * srcs], refs[2 * srcs:3 * srcs], refs[3 * srcs:4 * srcs], refs[4 * srcs:]
    (g1_ref, g3_ref), od_refs, (hot_buf, w_buf, od_buf, in_sem, out_sem) = refs[:2], refs[2:2 + srcs], refs[2 + srcs:]
    step, steps = pl.program_id(0), pl.num_programs(0)
    _, f = g1_ref.shape[1:]

    def loads(k):
        return [pltpu.make_async_copy(hot_refs[k], hot_buf.at[k], in_sem.at[2 * k]), pltpu.make_async_copy(w_refs[k], w_buf.at[k], in_sem.at[2 * k + 1])]

    def store(k):
        return pltpu.make_async_copy(od_buf.at[k], od_refs[k], out_sem.at[k])

    @pl.when(step == 0)
    def _():
        for k in range(srcs):
            for copy in loads(k):
                copy.start()

    for k in range(srcs):
        @pl.when(step == 2 + 2 * k)
        def _(k=k):
            for copy in loads(k):
                copy.wait()

    @pl.when((step >= 2) & (step < 2 + 2 * srcs) & (step % 2 == 0))
    def _():
        k = (step - 2) // 2
        hot_rows(hot_buf.at[k], w_buf.at[k], od_buf.at[k])

    for k in range(srcs):
        @pl.when(step == 2 + 2 * k)
        def _(k=k):
            store(k).start()

    for k in range(pair):
        expert = step * pair + k
        x = load_rows(x_refs, tbl_ref, expert)
        dab = jnp.concatenate([dab_refs[s][pl.ds(window(tbl_ref, s, expert, dab_refs[s].shape[0])[0], WIN), :] for s in range(srcs)], axis=0)
        g13 = mm_tn(x, dab)
        g1_ref[k] = g13[:, :f]
        g3_ref[k] = g13[:, f:]

    @pl.when(step == steps - 1)
    def _():
        for k in range(srcs):
            store(k).wait()


def hot_weight_kernel(w1_ref, w3_ref, w2_ref, after_ref, out_ref):
    del after_ref
    f = w1_ref.shape[2]
    out_ref[:, :f] = w1_ref[0]
    out_ref[:, f:2 * f] = w3_ref[0]
    for j in range(w2_ref.shape[2] // f):
        out_ref[j * f:(j + 1) * f, 2 * f:] = w2_ref[0, :, j * f:(j + 1) * f]


def hot_rows(xg_ref, w_ref, od_ref):
    d = xg_ref.shape[1] // 2
    f = w_ref.shape[1] // 3
    w1, w3 = w_ref[:, :f], w_ref[:, f:2 * f]
    w2 = jnp.concatenate([w_ref[j * f:(j + 1) * f, 2 * f:] for j in range(d // f)], axis=1)
    out, dx = second_stage(*elementwise(*first_stage(xg_ref[:, :d], xg_ref[:, d:], w1, w3, w2)), w1, w3, w2)
    od_ref[:, :d] = out
    od_ref[:, d:] = dx


def hot_grad_kernel(srcs, *refs):
    xg_refs, (w1_ref, w3_ref, w2_ref), refs = refs[:srcs], refs[srcs:srcs + 3], refs[srcs + 6:]
    (g1_ref, g3_ref, g2_ref), (buf, sem) = refs[:3], refs[3:]
    d = w1_ref.shape[1]
    copies = [pltpu.make_async_copy(xg_refs[k], buf.at[k], sem.at[k]) for k in range(srcs)]
    for copy in copies:
        copy.start()
    for ref in (g1_ref, g3_ref, g2_ref):
        ref[...] = jnp.zeros_like(ref)
    for copy in copies:
        copy.wait()

    def add(k, _):
        x, g = buf[k, :, :d], buf[k, :, d:]
        h, da, db = elementwise(*first_stage(x, g, w1_ref[0], w3_ref[0], w2_ref[0]))
        g1_ref[0] += mm_tn(x, da)
        g3_ref[0] += mm_tn(x, db)
        g2_ref[0] += mm_tn(h, g)
        return 0

    lax.fori_loop(0, srcs, add, 0)


def combine_kernel(srcs, caps, sc_ref, vslot_ref, gate_ref, *refs):
    ret_refs, (y_ref, dx_ref, ret_ref, sem) = refs[:-4], refs[-4:]
    d = y_ref.shape[1]

    @pl.when(pl.program_id(0) == 0)
    def _():
        copies, at = [], 0
        for i, ref in enumerate(ret_refs):
            rows = ref.shape[0]
            copies.append(pltpu.make_async_copy(ref, ret_ref.at[pl.ds(at, rows)], sem.at[i]))
            at += rows
        for copy in copies:
            copy.start()
        for copy in copies:
            copy.wait()

    vslot = to_column(vslot_ref[...].astype(F32))
    lane = iota((1, ret_ref.shape[0]), 1)
    have, at = lane, 0
    for i, ref in enumerate(ret_refs):
        kind, off = divmod(i, srcs)
        base = (kind * srcs + (sc_ref[1] ^ off)) * LIST + sc_ref[0] * caps[kind] - at
        have = jnp.where(lane >= at, lane + base, have)
        at += ref.shape[0]
        have = jnp.where((lane >= at - ref.shape[0] + caps[kind]) & (lane < at), -2, have)
    pick = jnp.where(have.astype(F32) == vslot, 1.0, 0.0).astype(BF16)
    y_ref[...] = (to_column(gate_ref[...]) * mm(pick, ret_ref[:, :d])).astype(BF16)
    dx_ref[...] = mm(pick, ret_ref[:, d:]).astype(BF16)


def kernel_call(body, **options):
    return pl.pallas_call(body, **options)


def params(mib):
    return pltpu.CompilerParams(vmem_limit_bytes=mib * 2 ** 20, dimension_semantics=('arbitrary',))


def cost(flops, nbytes):
    return pl.CostEstimate(flops=int(flops), bytes_accessed=int(nbytes), transcendentals=0)


def prefetched(grid, in_specs, out_specs, scratch=()):
    return pltpu.PrefetchScalarGridSpec(num_scalar_prefetch=1, grid=grid, in_specs=in_specs, out_specs=out_specs, scratch_shapes=list(scratch))


COLD_SLAB, COLD_CAP, HOT_SLAB, PAIR, COLD_PAIR = 272, 271, 288, 4, 4


def solution(mesh):
    srcs = mesh.shape['expert']
    tok_spec = P(('data', 'expert'))
    weight_spec = P('expert')
    whole = functools.partial(pl.BlockSpec, pipeline_mode=pl.Buffered(1))
    sds = jax.ShapeDtypeStruct

    def shard_body(tok_x, route_idx, route_gate, grad_y, w_gate, w_up, w_down):
        tok_n, d = tok_x.shape
        local_n, _, f = w_gate.shape
        capacity = max(4, 2 * tok_n // (local_n * srcs))
        ids_row = route_idx.reshape(1, tok_n)
        gate_row = route_gate.reshape(1, tok_n)
        w_bytes = local_n * 3 * d * f * 2
        hot_rows = srcs * HOT_SLAB

        me = lax.axis_index('expert').astype(I32)
        flat = lambda *_: (0, 0)
        row_spec, tbl_spec, tok_spec_in = whole((1, tok_n), flat), whole((8, 256), flat), whole((tok_n, d), flat)

        def pack(kernel, sc, ins, in_specs, outs, name, scratch=()):
            return kernel_call(
                kernel,
                grid_spec=prefetched((1,), in_specs, [whole(o, flat) for o in outs], scratch),
                out_shape=[sds(o, BF16) for o in outs],
                compiler_params=params(62),
                cost_estimate=cost(2 * sum(o[0] * o[1] for o in outs) * tok_n, 4 * tok_n * d),
                name=name,
            )(sc, *ins)

        def send(value, k):
            return lax.ppermute(value, 'expert', [(i, i ^ k) for i in range(srcs)])

        def exchange(rows):
            return [rows[0]] + [send(rows[k], k) for k in range(1, srcs)]

        def swap(one):
            far = send(one, 2)
            return [one, send(one, 1), far, send(far, 1)]

        def combine(sc, vslot, rets):
            blk = pl.BlockSpec((256, d), lambda i, t: (i, 0))
            row = pl.BlockSpec((1, 256), lambda i, t: (0, i))
            total = sum(r.shape[0] for r in rets)
            return kernel_call(
                functools.partial(combine_kernel, srcs, (COLD_CAP, HOT_SLAB)),
                grid_spec=prefetched((tok_n // 256,), [row, row] + [pl.BlockSpec(memory_space=pl.ANY)] * len(rets), [blk, blk], [pltpu.VMEM((total, 2 * d), BF16), pltpu.SemaphoreType.DMA((len(rets),))]),
                out_shape=[sds((tok_n, d), BF16), sds((tok_n, d), BF16)],
                compiler_params=params(24),
                cost_estimate=cost(2 * tok_n * total * 2 * d, total * 2 * d * 4),
                name='combine',
            )(sc, vslot, gate_row, *rets)

        def one_round(rnd, pair, wide):
            sc = jnp.concatenate([rnd, me[None]])
            far, near = (2, 3), (0, 1)
            cold, hot = (COLD_SLAB, d), (HOT_SLAB, 2 * d)
            any_spec = pl.BlockSpec(memory_space=pl.ANY)
            caps = (COLD_CAP, HOT_SLAB)
            vslot, tbl, *x_far = kernel_call(
                functools.partial(route_kernel, capacity, caps, far),
                grid_spec=prefetched((1,), [row_spec, any_spec], [row_spec, tbl_spec] + [whole(cold, flat)] * 2, [pltpu.VMEM((1, tok_n), F32), pltpu.VMEM((tok_n, d), BF16), pltpu.SemaphoreType.DMA(())]),
                out_shape=[sds((1, tok_n), I32), sds((8, 256), F32)] + [sds(cold, BF16)] * 2,
                compiler_params=params(62),
                cost_estimate=cost(2 * 2 * COLD_SLAB * d * tok_n, 4 * tok_n * d),
                name='route',
            )(sc, ids_row, tok_x)
            grad_g, *g_far = pack(functools.partial(pack_g_kernel, far, COLD_CAP), sc, (vslot, gate_row, grad_y), [row_spec, row_spec, tok_spec_in], [(tok_n, d)] + [cold] * 2, 'pack_g', [pltpu.VMEM(cold, F32)])
            rest = pack(functools.partial(pack_rest_kernel, near, srcs, caps), sc, (vslot, tbl, tok_x, grad_g), [row_spec, tbl_spec, tok_spec_in, tok_spec_in], [cold] * 4 + [hot] * srcs, 'pack_rest', [pltpu.VMEM(hot, F32)])
            cold_x = exchange(list(rest[:2]) + list(x_far))
            cold_g = exchange(list(rest[2:4]) + list(g_far))
            hot_send = list(rest[4:])
            hot_xg = exchange(hot_send)
            last = pl.BlockSpec((16, 256), lambda i, t: (COLD_SLAB // 16 - 1, 0))
            win_tbl, rounds = kernel_call(
                functools.partial(table_kernel, COLD_CAP, local_n),
                grid_spec=prefetched((1,), [last] * srcs, [whole((srcs, 2 * local_n), flat), whole((1, 128), flat)]),
                out_shape=[sds((srcs, 2 * local_n), I32), sds((1, 128), I32)],
                compiler_params=params(62),
                name='table',
            )(sc, *cold_x)

            first = lambda *_: (0, 0, 0)
            w13_0, w2_0 = whole((1, d, f), first), whole((1, f, d), first)
            slab_spec = whole((COLD_SLAB, 2 * d), flat)
            x_spec = whole((COLD_SLAB, d), flat)
            dab_spec = whole((COLD_SLAB, 2 * f), flat)
            w13 = pl.BlockSpec((pair, d, f), lambda i, t: (i, 0, 0))
            w2 = pl.BlockSpec((pair, f, d), lambda i, t: (i, 0, 0))
            wide_w = [pl.BlockSpec((wide, d, f), lambda i, t: (i, 0, 0))] * 2 + [pl.BlockSpec((wide, f, d), lambda i, t: (i, 0, 0))]
            *res, grad2 = kernel_call(
                functools.partial(cold_kernel, srcs, wide),
                grid_spec=prefetched((local_n // wide,), [x_spec] * (2 * srcs) + [*wide_w], [slab_spec] * srcs + [dab_spec] * srcs + wide_w[2:]),
                out_shape=[sds((COLD_SLAB, 2 * d), BF16)] * srcs + [sds((COLD_SLAB, 2 * f), BF16)] * srcs + [sds((local_n, f, d), F32)],
                compiler_params=params(62),
                cost_estimate=cost(2 * 7 * 512 * local_n * d * f, w_bytes),
                name='cold',
            )(win_tbl, *cold_x, *cold_g, w_gate, w_up, w_down)
            cold_od, cold_dab = res[:srcs], res[srcs:]
            cold_ret = exchange(cold_od)

            hot_w = kernel_call(
                hot_weight_kernel,
                grid=(1,),
                in_specs=[w13_0, w13_0, w2_0, whole((16, 128), flat)],
                out_specs=whole((d, 3 * f), flat),
                out_shape=sds((d, 3 * f), BF16),
                compiler_params=params(62),
                name='hot_weight',
            )(w_gate, w_up, w_down, hot_send[0])
            hot_w = swap(hot_w)
            grad1, grad3, *hot_od = kernel_call(
                functools.partial(grad_kernel, srcs, pair),
                grid_spec=prefetched(
                    (local_n // pair,),
                    [x_spec] * srcs + [dab_spec] * srcs + [any_spec] * (2 * srcs),
                    [w13, w13] + [any_spec] * srcs,
                    [pltpu.VMEM((srcs, HOT_SLAB, 2 * d), BF16), pltpu.VMEM((srcs, d, 3 * f), BF16), pltpu.VMEM((srcs, HOT_SLAB, 2 * d), BF16), pltpu.SemaphoreType.DMA((2 * srcs,)), pltpu.SemaphoreType.DMA((srcs,))],
                ),
                out_shape=[sds((local_n, d, f), F32)] * 2 + [sds((HOT_SLAB, 2 * d), BF16)] * srcs,
                compiler_params=params(62),
                cost_estimate=cost(2 * 2 * 512 * local_n * d * f, 2 * w_bytes),
                name='grads',
            )(win_tbl, *cold_x, *cold_dab, *hot_send, *hot_w)

            grads = kernel_call(
                functools.partial(hot_grad_kernel, srcs),
                grid=(1,),
                in_specs=[any_spec] * srcs + [w13_0, w13_0, w2_0] + [any_spec] * 3,
                scratch_shapes=[pltpu.VMEM((srcs, HOT_SLAB, 2 * d), BF16), pltpu.SemaphoreType.DMA((srcs,))],
                out_specs=[w13_0, w13_0, w2_0],
                out_shape=[sds((local_n, d, f), F32), sds((local_n, d, f), F32), sds((local_n, f, d), F32)],
                input_output_aliases={srcs + 3: 0, srcs + 4: 1, srcs + 5: 2},
                compiler_params=params(26),
                cost_estimate=cost(2 * 6 * hot_rows * d * f, 4 * hot_rows * d * 4),
                name='hot_grads',
            )(*hot_xg, w_gate, w_up, w_down, grad1, grad3, grad2)

            y, dx = combine(sc, vslot, cold_ret + list(hot_od))
            return rounds[0, 0], (y, dx, *grads)

        rounds, outs = one_round(jnp.zeros((1,), I32), PAIR, COLD_PAIR)

        def more(state):
            return state[0][0] < rounds

        def again(state):
            _, extra = one_round(state[0], 1, 1)
            return (state[0] + 1, *(a + b for a, b in zip(state[1:], extra)))

        return lax.while_loop(more, again, (jnp.ones((1,), I32), *outs))[1:]

    return jax.shard_map(shard_body, mesh=mesh, in_specs=(tok_spec, tok_spec, tok_spec, tok_spec, weight_spec, weight_spec, weight_spec), out_specs=(tok_spec,) * 5, check_vma=False)
```
